512 devices in a mesh: group: 2 (over y), expert: 32 (over z), tensor: 4 (over x), sub: 2 (over core).
Axes of the slice: x: 4, y: 2, z: 32, core: 2. Of those that a mesh axis runs over, the one named last changes fastest.
The devices are a block of a 4x16x32 slice.
Arguments:
- tokens: bfloat16 [512, 7168], P(('group', 'expert', 'sub')), parts along dimension 0, may hold values from -6 to 6
- expert_ids: int32 [512, 8], P(('group', 'expert', 'sub')), parts along dimension 0, may hold values from 0 to 15, all different within a row; in each aligned block of 4 rows (0 to 3, 4 to 7, ...) at most 3 rows name the same one
- gate_codes: int32 [512, 8], P(('group', 'expert', 'sub')), parts along dimension 0, may hold values from 1 to 63
- w_gate: bfloat16 [32, 1024, 7168], P('expert', ('tensor', 'sub')), may hold values from -0.0625 to 0.0625
- w_up: bfloat16 [32, 1024, 7168], P('expert', ('tensor', 'sub')), may hold values from -0.0625 to 0.0625
- w_down: bfloat16 [32, 1024, 7168], P('expert', ('tensor', 'sub')), may hold values from -0.125 to 0.125
Outputs:
- mixed: bfloat16 [512, 7168], P(('group', 'expert', 'sub'), 'tensor'), parts along dimension 0
The draws below stay inside these ranges and needn't reach their ends.
There are 2 independent parts, one for each index of `group`. The reference program is written for one: setup_inputs(seed, part) draws one part's arguments, and reference() takes and returns one part's arrays. A program takes and returns all parts, laid end to end along the dimension named above; an argument that names none is the same for every part. Nothing has to cross between parts.
Inputs may be any that keep to these rules, and one draw needn't show every extreme that they name: `expert_ids`: the 8 numbers of a row differ; within the rows of one device (aligned blocks of 4 rows) no expert is named by more than 3 rows, a bound that some block reaches.
All inputs are finite; a program needn't handle non-finite values.
Results may differ from the reference program's by a relative error of at most 0.008.
Values may be sent and summed in bfloat16 or wider, within the bound.
No kernel may reach another device: no remote copies, remote signals or barrier semaphores. Data moves between devices by JAX's collectives and lax.ppermute only.
A program may use at most 64 MiB of HBM per device.

```python
import math
import jax
import jax.numpy as jnp
import numpy as np
from jax import lax

D = 7168
FF = 2048
TOK_DEV = 4
EXPERTS = 16
HALVES = 32
TOP = 8
CAP = 3
RUN = 128
TOKENS = 256


def set_ends(drawn, rng, smallest, high):
    spot = [jax.random.randint(jax.random.fold_in(rng, axis), (), 0, length) for axis, length in enumerate(drawn.shape)]
    widest = drawn.shape.index(max(drawn.shape))
    next_to = spot[:widest] + [(spot[widest] + 1) % drawn.shape[widest]] + spot[widest + 1:]
    return drawn.at[tuple(spot)].set(smallest).at[tuple(next_to)].set(high)


def block_scale(key, extent, cuts, low, top_value):
    def one(position, parts):
        steps = jax.random.uniform(jax.random.fold_in(jax.random.fold_in(key, 6), position), (parts,), jnp.float32, low / len(cuts), top_value / len(cuts))
        return jnp.repeat(jnp.exp(steps), extent[position] // parts).reshape((-1,) + (1,) * (len(extent) - position - 1))

    factor_of = one(*cuts[0])
    for cut in cuts[1:]:
        factor_of = factor_of * one(*cut)
    return factor_of


def deal_out(key, own, number, rows, count, top, bound, lean):
    ranking = jax.random.permutation(key, count)
    heavy_load, usual = load_shares(count, rows * top, bound, lean, True), load_shares(count, rows * top, bound, lean, False)
    places = jnp.arange(count)

    def named(tallies, turn):
        used = int((tallies > 0).sum())
        fixed = max(1, used // 4)
        moved = fixed + (places - fixed + turn * (used - fixed)) % max(1, count - fixed)
        return jnp.zeros((count,), jnp.int32).at[ranking[jnp.where(places < fixed, places, moved)]].set(jnp.asarray(tallies, jnp.int32))

    tallies = jnp.where(number % 4 == 0, named(heavy_load, number // 4), named(usual, number - number // 4 - 1))
    mixed = jax.random.permutation(jax.random.fold_in(own, 3), count)
    giver, receiver = mixed[0:count // 2 * 2:2], mixed[1:count // 2 * 2:2]
    slack = jnp.minimum(tallies[giver] - 1, bound - tallies[receiver]) // 2
    slack = jnp.where((giver == ranking[0]) | (receiver == ranking[0]) | (tallies[receiver] == 0), 0, jnp.maximum(slack, 0))
    moved = jax.random.randint(jax.random.fold_in(own, 4), (count // 2,), 0, 1 << 20) % (slack + 1)
    tallies = tallies.at[giver].add(-moved).at[receiver].add(moved)
    items = jnp.searchsorted(jnp.cumsum(tallies), jnp.arange(rows * top), side="right").astype(jnp.int32)
    table = items.reshape(top, rows).T
    table = table[jax.random.permutation(jax.random.fold_in(own, 1), rows)]
    turn = jax.random.randint(jax.random.fold_in(own, 2), (rows, 1), 0, top)
    return jnp.take_along_axis(table, (jnp.arange(top)[None, :] + turn) % top, axis=1)


def load_shares(count, total, bound, skew, full):
    loads = [(1 << 20) // math.isqrt(rank ** skew) + 1 for rank in range(1, count + 1)]
    largest = bound if full else min(bound, max(-(-total // count), total * loads[0] // sum(loads)))
    least = 1 if total - largest >= count - 1 else 0
    counts, spare = [largest] + [least] * (count - 1), total - largest - least * (count - 1)
    while spare > 0:
        candidates = [i for i in range(1, count) if counts[i] < largest] or [i for i in range(1, count) if counts[i] < bound]
        pool, left = sum([loads[i] for i in candidates]), spare
        for i in candidates:
            more = min(bound - counts[i], max(1, left * loads[i] // pool), spare)
            counts[i] = counts[i] + more
            spare = spare - more
    return np.array(counts)


def normal_values(own_key, dims, deviation, most, pieces=(), held_as=jnp.bfloat16):
    gain = block_scale(own_key, dims, pieces, -0.22, 0.18) if pieces else 1.0
    drawn = jax.random.normal(own_key, dims, jnp.float32) * deviation * gain
    return jnp.minimum(jnp.maximum(drawn, -most), most).astype(held_as)


def setup_inputs(seed: int = 0, part: int = 0) -> dict:
    arg_keys = jax.random.split(jax.random.key(seed), 7)
    part_keys = jax.random.split(jax.random.fold_in(arg_keys[6], part), 7)
    tokens = normal_values(part_keys[0], (TOKENS, D), 1.0, 6.0, ((0, 64),))
    expert_ids_keys = jax.random.split(jax.random.fold_in(part_keys[1], 1), TOKENS // TOK_DEV)
    expert_ids_turns = jax.random.permutation(jax.random.fold_in(part_keys[1], 3), TOKENS // TOK_DEV)
    expert_ids = jax.vmap(lambda own, number: deal_out(jax.random.fold_in(part_keys[1], 2), own, number, TOK_DEV, EXPERTS, TOP, CAP, 1))(expert_ids_keys, expert_ids_turns).reshape((TOKENS, TOP))
    gate_codes = set_ends(jax.random.randint(part_keys[2], (TOKENS, TOP), 1, 64), jax.random.fold_in(part_keys[2], 1), 1, 63).astype(jnp.int32)
    w_gate = normal_values(arg_keys[3], (HALVES, FF // 2, D), D ** -0.5, 0.0625, ((0, 32), (1, 8)))
    w_up = normal_values(arg_keys[4], (HALVES, FF // 2, D), D ** -0.5, 0.0625, ((0, 32), (1, 8)))
    w_down = normal_values(arg_keys[5], (HALVES, FF // 2, D), FF ** -0.5, 0.125, ((0, 32), (1, 8)))
    return dict(tokens=tokens, expert_ids=expert_ids, gate_codes=gate_codes, w_gate=w_gate, w_up=w_up, w_down=w_down)


def reference(tokens, expert_ids, gate_codes, w_gate, w_up, w_down):
    weight = gate_codes.astype(jnp.float32) / 64.0
    token_count = tokens.shape[0]
    run_count = FF // RUN
    contract = (((1,), (1,)), ((), ()))

    def one_expert(total_out, expert):
        gate_full = jnp.concatenate([w_gate[2 * expert], w_gate[2 * expert + 1]], axis=0)
        up_full = jnp.concatenate([w_up[2 * expert], w_up[2 * expert + 1]], axis=0)
        down_full = jnp.concatenate([w_down[2 * expert], w_down[2 * expert + 1]], axis=0)
        gate_act = lax.dot_general(tokens, gate_full, contract, preferred_element_type=jnp.float32)
        up_act = lax.dot_general(tokens, up_full, contract, preferred_element_type=jnp.float32)
        hidden = (jax.nn.silu(gate_act) * up_act).astype(jnp.bfloat16)
        hid_runs = hidden.reshape(token_count, run_count, RUN).transpose(1, 0, 2)
        down_runs = down_full.reshape(run_count, RUN, D)

        def add_run(running, run_pair):
            hid_run, down_run = run_pair
            piece = jnp.dot(hid_run, down_run, preferred_element_type=jnp.float32).astype(jnp.bfloat16)
            piece = lax.optimization_barrier(piece)
            return running + piece.astype(jnp.float32), None

        summed, _ = lax.scan(add_run, jnp.zeros((token_count, D), jnp.float32), (hid_runs, down_runs))
        share_of = jnp.sum(jnp.where(expert_ids == expert, weight, jnp.float32(0.0)), axis=1)
        return total_out + share_of[:, None] * summed, None

    total_out, _ = lax.scan(one_expert, jnp.zeros((token_count, D), jnp.float32), jnp.arange(EXPERTS, dtype=jnp.int32))
    return total_out.astype(jnp.bfloat16)
```

```python
import functools

import jax
import jax.numpy as jnp
from jax import lax
from jax.experimental import pallas as pl
from jax.experimental.pallas import tpu as pltpu
from jax.sharding import PartitionSpec as P

BF = jnp.bfloat16
F32 = jnp.float32
VM = pl.BlockSpec(memory_space=pltpu.VMEM)
CONTRACT = (((1,), (1,)), ((), ()))


def hidden_kernel(x_ref, g_ref, u_ref, h_ref):
    parts, rows, block = x_ref.shape
    gate = jnp.zeros((rows, g_ref.shape[0]), F32)
    up = jnp.zeros((rows, u_ref.shape[0]), F32)
    for k in range(parts):
        cols = pl.ds(k * block, block)
        x = x_ref[k]
        gate += lax.dot_general(x, g_ref[:, cols], CONTRACT, preferred_element_type=F32)
        up += lax.dot_general(x, u_ref[:, cols], CONTRACT, preferred_element_type=F32)
    h_ref[...] = (gate / (1.0 + jnp.exp(-gate)) * up).astype(h_ref.dtype)


def hidden_of(x, g, u):
    parts, rows, block = x.shape
    units = g.shape[0]
    return pl.pallas_call(
        hidden_kernel,
        out_shape=jax.ShapeDtypeStruct((rows, units), BF),
        in_specs=[VM] * 3,
        out_specs=VM,
        cost_estimate=pl.CostEstimate(
            flops=4 * rows * units * parts * block,
            bytes_accessed=2 * (rows + 2 * units) * parts * block,
            transcendentals=rows * units,
        ),
        name="hidden",
    )(x, g, u)


def down_kernel(h_ref, d_ref, o_ref):
    parts, rows, block = o_ref.shape
    h = h_ref[...]
    for k in range(parts):
        o_ref[k] = jnp.dot(
            h, d_ref[:, pl.ds(k * block, block)], preferred_element_type=F32
        ).astype(o_ref.dtype)


def down_add_kernel(h_ref, d_ref, a_ref, o_ref):
    parts, rows, block = o_ref.shape
    h = h_ref[...]
    for k in range(parts):
        own = jnp.dot(h, d_ref[:, pl.ds(k * block, block)], preferred_element_type=F32)
        o_ref[k] = (own + a_ref[k].astype(F32)).astype(o_ref.dtype)


def down_of(h, d, parts, other=None):
    rows, units = h.shape
    block = d.shape[1] // parts
    args = (h, d) if other is None else (h, d, other)
    return pl.pallas_call(
        down_kernel if other is None else down_add_kernel,
        out_shape=jax.ShapeDtypeStruct((parts, rows, block), BF),
        in_specs=[VM] * len(args),
        out_specs=VM,
        cost_estimate=pl.CostEstimate(
            flops=2 * rows * units * parts * block,
            bytes_accessed=2 * (rows + units) * parts * block,
            transcendentals=0,
        ),
        name="down" if other is None else "down_add",
    )(*args)


def shards(tokens, expert_ids, gate_codes, w_gate, w_up, w_down):
    rows, features = tokens.shape
    per_token = expert_ids.shape[1]
    owners = lax.axis_size("expert")
    subs = lax.axis_size("sub")
    parts = lax.axis_size("tensor")
    experts = owners // 2
    capacity = min(rows, rows * per_token // experts + 1)
    block = features // parts
    half = block // 2
    here = lax.axis_index("tensor")
    odd = lax.axis_index("expert") % 2
    swap_sub = [(i, subs - 1 - i) for i in range(subs)]
    swap_pair = [(i, i ^ 1) for i in range(owners)]

    picks = expert_ids[:, :, None] == jnp.arange(experts, dtype=jnp.int32)
    named = jnp.any(picks, axis=1)
    weight = jnp.sum(jnp.where(picks, gate_codes[:, :, None].astype(F32) / 64.0, 0.0), axis=1)
    count = named.astype(jnp.int32)
    slot = [jnp.zeros((experts,), jnp.int32)]
    for t in range(1, rows):
        slot.append(slot[-1] + count[t - 1])
    slot = jnp.stack(slot)
    onehot = named[:, :, None] & (slot[:, :, None] == jnp.arange(capacity, dtype=jnp.int32))
    combine = jnp.where(onehot, weight[:, :, None], 0.0)

    mine = lax.dynamic_slice(tokens, (0, here * block), (rows, block))
    packed = jnp.einsum("tes,tpf->epsf", onehot.astype(BF), mine.reshape(rows, 2, half)).astype(BF)
    arrived = lax.all_to_all(
        packed.reshape(owners, capacity, half), "expert", split_axis=0, concat_axis=0, tiled=True
    )
    slots = owners * capacity
    arrived = arrived.reshape(slots, half)
    partner = lax.ppermute(arrived, "expert", swap_pair)
    low = jnp.where(odd == 0, arrived, partner)
    high = jnp.where(odd == 0, partner, arrived)
    quarter = jnp.concatenate([low, high], axis=1)
    own_rows = lax.all_to_all(
        jnp.broadcast_to(quarter[None], (parts, slots, block)),
        "tensor",
        split_axis=0,
        concat_axis=0,
        tiled=True,
    )
    other_rows = lax.ppermute(own_rows, "sub", swap_sub)
    own_hidden = hidden_of(own_rows, w_gate[0], w_up[0])
    other_hidden = hidden_of(other_rows, w_gate[0], w_up[0])
    other_part = down_of(other_hidden, w_down[0], parts)
    from_other = lax.ppermute(other_part, "sub", swap_sub)
    part = down_of(own_hidden, w_down[0], parts, from_other)
    gathered = lax.all_to_all(part, "tensor", split_axis=0, concat_axis=0, tiled=True)
    total = jnp.sum(gathered.astype(F32), axis=0)
    keep = jnp.where(odd == 0, total[:, :half], total[:, half:])
    give = jnp.where(odd == 0, total[:, half:], total[:, :half]).astype(BF)
    taken = lax.ppermute(give, "expert", swap_pair)
    both = (keep + taken.astype(F32)).astype(BF).reshape(owners, capacity, half)
    back = lax.all_to_all(both, "expert", split_axis=0, concat_axis=0, tiled=True)
    back = back.reshape(experts, 2, capacity, half).astype(F32)
    mixed = jnp.einsum(
        "tes,epsf->tpf", combine, back, precision=lax.Precision.HIGHEST, preferred_element_type=F32
    )
    return mixed.reshape(rows, block).astype(BF)


def solution(mesh):
    spread = P(("group", "expert", "sub"), None)
    weights = P("expert", ("tensor", "sub"), None)
    return jax.shard_map(
        shards,
        mesh=mesh,
        in_specs=(spread, spread, spread, weights, weights, weights),
        out_specs=P(("group", "expert", "sub"), "tensor"),
        check_vma=False,
    )
```

```python
import jax
import jax.numpy as jnp
from jax import lax
from jax.experimental import pallas as pl
from jax.experimental.pallas import tpu as pltpu
from jax.sharding import PartitionSpec as P

BF = jnp.bfloat16
F32 = jnp.float32
VM = pl.BlockSpec(memory_space=pltpu.VMEM)
SM = pl.BlockSpec(memory_space=pltpu.SMEM)
CONTRACT = (((1,), (1,)), ((), ()))


def expert_kernel(odd_ref, x0_ref, x1_ref, g0, u0, d0, g1, u1, d1, keep_ref, give_ref):
    parts, rows, half = x0_ref.shape
    odd = odd_ref[0]

    def cols(k, other):
        which = 1 - odd if other else odd
        return pl.ds(pl.multiple_of((2 * k + which) * half, 128), half)

    hidden = []
    for g, u in ((g0, u0), (g1, u1)):
        gate = jnp.zeros((rows, g.shape[0]), F32)
        up = jnp.zeros((rows, u.shape[0]), F32)
        for k in range(parts):
            for other, x_ref in ((False, x0_ref), (True, x1_ref)):
                x = x_ref[k]
                at = cols(k, other)
                gate += lax.dot_general(x, g[:, at], CONTRACT, preferred_element_type=F32)
                up += lax.dot_general(x, u[:, at], CONTRACT, preferred_element_type=F32)
        hidden.append((gate / (1.0 + jnp.exp(-gate)) * up).astype(BF))
    for other, o_ref in ((True, give_ref), (False, keep_ref)):
        for k in range(parts):
            at = cols(k, other)
            total = jnp.dot(hidden[0], d0[:, at], preferred_element_type=F32)
            total += jnp.dot(hidden[1], d1[:, at], preferred_element_type=F32)
            o_ref[k] = total.astype(BF)


def experts_of(odd, x0, x1, own, other):
    parts, rows, half = x0.shape
    units, features = own[0].shape
    shape = jax.ShapeDtypeStruct((parts, rows, half), BF)
    return pl.pallas_call(
        expert_kernel,
        out_shape=(shape, shape),
        in_specs=[SM] + [VM] * 8,
        out_specs=(VM, VM),
        cost_estimate=pl.CostEstimate(
            flops=12 * rows * units * features,
            bytes_accessed=12 * units * features + 4 * rows * features,
            transcendentals=2 * rows * units,
        ),
        compiler_params=pltpu.CompilerParams(vmem_limit_bytes=24 * 1024 * 1024),
        name="experts",
    )(odd, x0, x1, *own, *other)


def shards(tokens, expert_ids, gate_codes, w_gate, w_up, w_down):
    rows, features = tokens.shape
    per_token = expert_ids.shape[1]
    owners = lax.axis_size("expert")
    subs = lax.axis_size("sub")
    parts = lax.axis_size("tensor")
    experts = owners // 2
    capacity = min(rows, rows * per_token // experts + 1)
    slots = owners * capacity
    block = features // parts
    half = block // 2
    here = lax.axis_index("tensor")
    odd = lax.axis_index("expert") & 1
    swap_sub = [(i, subs - 1 - i) for i in range(subs)]
    swap_pair = [(i, i ^ 1) for i in range(owners)]

    own = (w_gate[0], w_up[0], w_down[0])
    other = [lax.ppermute(w, "sub", swap_sub) for w in own]

    picks = expert_ids[:, :, None] == jnp.arange(experts, dtype=jnp.int32)
    named = jnp.any(picks, axis=1)
    weight = jnp.sum(jnp.where(picks, gate_codes[:, :, None].astype(F32) / 64.0, 0.0), axis=1)
    count = named.astype(jnp.int32)
    slot = [jnp.zeros((experts,), jnp.int32)]
    for t in range(1, rows):
        slot.append(slot[-1] + count[t - 1])
    slot = jnp.stack(slot)
    onehot = named[:, :, None] & (slot[:, :, None] == jnp.arange(capacity, dtype=jnp.int32))
    combine = jnp.where(onehot, weight[:, :, None], 0.0)

    mine = lax.dynamic_slice(tokens, (0, here * block), (rows, block))
    packed = jnp.einsum("tes,tpf->epsf", onehot.astype(BF), mine.reshape(rows, 2, half)).astype(BF)
    arrived = lax.all_to_all(
        packed.reshape(owners, capacity, half), "expert", split_axis=0, concat_axis=0, tiled=True
    )
    arrived = arrived.reshape(slots, half)
    partner = lax.ppermute(arrived, "expert", swap_pair)

    def across(x):
        return lax.all_to_all(x, "tensor", split_axis=0, concat_axis=0, tiled=True)

    x0 = across(jnp.broadcast_to(arrived[None], (parts, slots, half)))
    x1 = across(jnp.broadcast_to(partner[None], (parts, slots, half)))
    keep, give = experts_of(odd.reshape(1), x0, x1, own, other)
    give = jnp.sum(across(give).astype(F32), axis=0).astype(BF)
    taken = lax.ppermute(give, "expert", swap_pair)
    keep = jnp.sum(across(keep).astype(F32), axis=0)
    both = (keep + taken.astype(F32)).astype(BF).reshape(owners, capacity, half)
    back = lax.all_to_all(both, "expert", split_axis=0, concat_axis=0, tiled=True)
    back = back.reshape(experts, 2, capacity, half).astype(F32)
    mixed = jnp.einsum(
        "tes,epsf->tpf", combine, back, precision=lax.Precision.HIGHEST, preferred_element_type=F32
    )
    return mixed.reshape(rows, block).astype(BF)


def solution(mesh):
    spread = P(("group", "expert", "sub"), None)
    weights = P("expert", ("tensor", "sub"), None)
    return jax.shard_map(
        shards,
        mesh=mesh,
        in_specs=(spread, spread, spread, weights, weights, weights),
        out_specs=P(("group", "expert", "sub"), "tensor"),
        check_vma=False,
    )
```

```python
import jax
import jax.numpy as jnp
from jax import lax
from jax.experimental import pallas as pl
from jax.experimental.pallas import tpu as pltpu
from jax.sharding import PartitionSpec as P

BF = jnp.bfloat16
F32 = jnp.float32
I32 = jnp.int32
VM = pl.BlockSpec(memory_space=pltpu.VMEM)
SM = pl.BlockSpec(memory_space=pltpu.SMEM)
ANY = pl.BlockSpec(memory_space=pl.ANY)
CONTRACT = (((1,), (1,)), ((), ()))
MIB = 1024 * 1024


def params(mib):
    return pltpu.CompilerParams(vmem_limit_bytes=mib * MIB)


def split_of(half):
    return -(-half // 256) * 128


def routing(ids_ref, rows):
    row = lax.broadcasted_iota(I32, (rows, 1), 0)
    expert, side, part = row // 4, (row // 2) % 2, row % 2
    tokens, picks = ids_ref.shape
    count = jnp.zeros((rows, 1), I32)
    out = []
    for t in range(tokens):
        hits = [(expert == ids_ref[t, j]).astype(I32) for j in range(picks)]
        named = sum(hits)
        first = named * (count == part).astype(I32)
        third = named * (count == 2).astype(I32)
        out.append((hits, first, third))
        count = count + named
    return out, side, part


def pack_body(block, here_ref, ids_ref, tok_ref, o_ref):
    rows, width = o_ref.shape
    half = block // 2
    low = width - half
    routes, side, part = routing(ids_ref, rows)
    start = pl.multiple_of(here_ref[0] * block, 128)
    tok = tok_ref[:, pl.ds(start, block)].astype(F32)
    main = jnp.zeros((rows, half), F32)
    tail = jnp.zeros((rows, low), F32)
    for t, (_, first, third) in enumerate(routes):
        for p in range(2):
            piece = tok[t : t + 1, p * half : (p + 1) * half]
            here = (side == p).astype(I32)
            main = main + (first * here).astype(F32) * piece
            rest = piece[:, low:]
            if 2 * low > half:
                rest = jnp.concatenate([rest, jnp.zeros((1, 2 * low - half), F32)], axis=1)
            third_here = third * here
            tail = tail + (third_here * (1 - part)).astype(F32) * piece[:, :low]
            tail = tail + (third_here * part).astype(F32) * rest
    o_ref[:, :half] = main.astype(BF)
    o_ref[:, half:] = tail.astype(BF)


def packed_of(here, ids, tokens, owners, block):
    half = block // 2
    width = half + split_of(half)

    def kernel(*refs):
        pack_body(block, *refs)

    return pl.pallas_call(
        kernel,
        out_shape=jax.ShapeDtypeStruct((2 * owners, width), BF),
        in_specs=[SM, SM, VM],
        out_specs=VM,
        compiler_params=params(4),
        name="pack",
    )(here, ids, tokens)


def mix_kernel(ids_ref, code_ref, x_ref, o_ref):
    rows, width = x_ref.shape
    half = o_ref.shape[1] // 2
    low = width - half
    routes, side, part = routing(ids_ref, rows)
    x = x_ref[...].astype(F32)
    for t, (hits, first, third) in enumerate(routes):
        code = sum(hit * code_ref[t, j] for j, hit in enumerate(hits))
        weight = code.astype(F32) / 64.0
        for p in range(2):
            here = (side == p).astype(I32)

            def total(chosen, lo, hi):
                scaled = (chosen * here).astype(F32) * weight * x[:, lo:hi]
                return jnp.sum(scaled, axis=0, keepdims=True)

            main = total(first, 0, half)
            lower = total(third * (1 - part), half, width)
            upper = total(third * part, half, 2 * half - low)
            at = p * half
            o_ref[t : t + 1, at : at + low] = (main[:, :low] + lower).astype(BF)
            o_ref[t : t + 1, at + low : at + half] = (main[:, low:] + upper).astype(BF)


def mixed_of(ids, codes, x, block):
    return pl.pallas_call(
        mix_kernel,
        out_shape=jax.ShapeDtypeStruct((ids.shape[0], block), BF),
        in_specs=[SM, SM, VM],
        out_specs=VM,
        compiler_params=params(4),
        name="mix",
    )(ids, codes, x)


def fetch_kernel(g0, u0, d0, g1, u1, d1, g_ref, u_ref, d_ref, sems):
    copies = []
    for i, (src, dst) in enumerate(
        ((g0, g_ref), (u0, u_ref), (d0, d_ref), (g1, g_ref), (u1, u_ref), (d1, d_ref))
    ):
        units = src.shape[0]
        rows = pl.ds((i // 3) * units, units)
        copies.append(pltpu.make_async_copy(src, dst.at[rows], sems.at[i]))
    for copy in copies:
        copy.start()
    for copy in copies:
        copy.wait()


def fetched(own, other):
    units, features = own[0].shape
    shape = jax.ShapeDtypeStruct((2 * units, features), BF)
    return pl.pallas_call(
        fetch_kernel,
        out_shape=(shape,) * 3,
        in_specs=[ANY] * 6,
        out_specs=(VM,) * 3,
        scratch_shapes=[pltpu.SemaphoreType.DMA((6,))],
        cost_estimate=pl.CostEstimate(
            flops=12 * units * features * 256,
            bytes_accessed=24 * units * features,
            transcendentals=0,
        ),
        compiler_params=params(13),
        name="fetch",
    )(*(pltpu.with_memory_space_constraint(w, pltpu.MemorySpace.HBM) for w in own), *other)


def expert_kernel(here_ref, odd_ref, *refs):
    parts = (len(refs) - 5) // 2
    pieces, (g_ref, u_ref, d_ref, keep_ref, give_ref) = refs[: 2 * parts], refs[2 * parts :]
    owners, _, width = pieces[0].shape
    rows = 2 * owners
    half = d_ref.shape[1] // (2 * parts)
    low = width - half
    units = g_ref.shape[0]
    odd, here = odd_ref[0], here_ref[0]

    def start(k, other):
        side = 1 - odd if other else odd
        return pl.multiple_of((2 * k + side) * half, 128)

    sums = [[jnp.zeros((2 * rows, units), F32) for _ in range(2)] for _ in range(2)]
    for i, x_ref in enumerate(pieces):
        k = lax.rem(here + parts - i % parts, parts)
        x = x_ref[...].reshape(rows, width)
        at = start(k, i >= parts)
        lhs = (
            jnp.concatenate([x[:, :low], x[:, half:]], axis=0),
            jnp.concatenate([x[:, low:half], x[:, half : 2 * half - low]], axis=0),
        )
        for w, w_ref in enumerate((g_ref, u_ref)):
            for c, (lo, size) in enumerate(((0, low), (low, half - low))):
                cols = pl.ds(pl.multiple_of(at + lo, 128), size)
                sums[w][c] += lax.dot_general(
                    lhs[c], w_ref[:, cols], CONTRACT, preferred_element_type=F32
                )

    def joined(a, b):
        third = a[rows:] + pltpu.roll(b[rows:], rows - 1, 0)
        return jnp.concatenate([a[:rows] + b[:rows], third], axis=0)

    gate, up = joined(*sums[0]), joined(*sums[1])
    hidden = gate / (1.0 + jnp.exp(-gate)) * up
    third = hidden[rows:]
    even = lax.broadcasted_iota(I32, (rows, units), 0) % 2 == 0
    lower = jnp.where(even, third, 0.0)
    upper = jnp.where(even, 0.0, pltpu.roll(third, 1, 0))
    lhs = (
        jnp.concatenate([hidden[:rows], lower], axis=0).astype(BF),
        jnp.concatenate([hidden[:rows], upper], axis=0).astype(BF),
    )
    for other, o_ref in ((True, give_ref), (False, keep_ref)):
        for k in range(parts):
            at = start(k, other)
            a = jnp.dot(lhs[0], d_ref[:, pl.ds(at, low)], preferred_element_type=F32)
            cols = pl.ds(pl.multiple_of(at + low, 128), half - low)
            b = jnp.dot(lhs[1], d_ref[:, cols], preferred_element_type=F32)
            o_ref[k, :, :low] = a[:rows].astype(BF)
            o_ref[k, :, low:half] = b[:rows].astype(BF)
            o_ref[k, :, half : 2 * half - low] = (a[rows:, : half - low] + b[rows:]).astype(BF)
            if 2 * low > half:
                o_ref[k, :, 2 * half - low :] = a[rows:, half - low :].astype(BF)


def experts_of(here, odd, pieces, weights):
    parts = len(pieces) // 2
    owners, _, width = pieces[0].shape
    units, features = weights[0].shape
    shape = jax.ShapeDtypeStruct((parts, 2 * owners, width), BF)
    return pl.pallas_call(
        expert_kernel,
        out_shape=(shape, shape),
        in_specs=[SM] * 2 + [VM] * (2 * parts + 3),
        out_specs=(VM, VM),
        cost_estimate=pl.CostEstimate(
            flops=24 * owners * units * features,
            bytes_accessed=6 * units * features,
            transcendentals=4 * owners * units,
        ),
        compiler_params=params(24),
        name="experts",
    )(here, odd, *pieces, *weights)


def shards(tokens, expert_ids, gate_codes, w_gate, w_up, w_down):
    rows, features = tokens.shape
    owners = lax.axis_size("expert")
    subs = lax.axis_size("sub")
    parts = lax.axis_size("tensor")
    experts = owners // 2
    assert min(rows, rows * expert_ids.shape[1] // experts + 1) == 3
    block = features // parts
    width = block // 2 + split_of(block // 2)
    here = lax.axis_index("tensor").reshape(1)
    odd = (lax.axis_index("expert") & 1).reshape(1)
    swap_sub = [(i, subs - 1 - i) for i in range(subs)]
    swap_pair = [(i, i ^ 1) for i in range(owners)]

    def turned(x, k):
        return lax.ppermute(x, "tensor", [(i, (i + k) % parts) for i in range(parts)])

    def across(x):
        return lax.all_to_all(x, "tensor", split_axis=0, concat_axis=0, tiled=True)

    def along(x):
        return lax.all_to_all(x, "expert", split_axis=0, concat_axis=0, tiled=True)

    own = (w_gate[0], w_up[0], w_down[0])
    other = [lax.ppermute(w, "sub", swap_sub) for w in own]
    weights = fetched(own, other)
    packed = packed_of(here, expert_ids, tokens, owners, block).reshape(owners, 2, width)
    arrived = along(packed)
    partner = lax.ppermute(arrived, "expert", swap_pair)
    pieces = [arrived] + [None] * (parts - 1) + [partner] + [None] * (parts - 1)
    steps = sorted(range(1, parts), key=lambda k: min(k, parts - k))
    for k in steps:
        pieces[k] = turned(arrived, k)
    for k in steps:
        pieces[parts + k] = turned(partner, k)
    keep, give = experts_of(here, odd, pieces, weights)
    give = across(give)
    give = jnp.sum(give.astype(F32), axis=0).astype(BF)
    taken = lax.ppermute(give, "expert", swap_pair)
    keep = across(keep)
    both = jnp.sum(keep.astype(F32), axis=0) + taken.astype(F32)
    both = both.astype(BF).reshape(owners, 2, width)
    back = along(both).reshape(2 * owners, width)
    return mixed_of(expert_ids, gate_codes, back, block)


def solution(mesh):
    spread = P(("group", "expert", "sub"), None)
    weights = P("expert", ("tensor", "sub"), None)
    return jax.shard_map(
        shards,
        mesh=mesh,
        in_specs=(spread, spread, spread, weights, weights, weights),
        out_specs=P(("group", "expert", "sub"), "tensor"),
        check_vma=False,
    )
```

```python
import jax
import jax.numpy as jnp
from jax import lax
from jax.experimental import pallas as pl
from jax.experimental.pallas import tpu as pltpu
from jax.sharding import PartitionSpec as P

BF = jnp.bfloat16
F32 = jnp.float32
I32 = jnp.int32
VM = pl.BlockSpec(memory_space=pltpu.VMEM)
SM = pl.BlockSpec(memory_space=pltpu.SMEM)
ANY = pl.BlockSpec(memory_space=pl.ANY)
CONTRACT = (((1,), (1,)), ((), ()))
MIB = 1024 * 1024


def params(mib):
    return pltpu.CompilerParams(vmem_limit_bytes=mib * MIB)


def split_of(half):
    return -(-half // 256) * 128


def routing(ids_ref, rows):
    row = lax.broadcasted_iota(I32, (rows, 1), 0)
    expert, side, part = row // 4, (row // 2) % 2, row % 2
    tokens, picks = ids_ref.shape
    count = jnp.zeros((rows, 1), I32)
    out = []
    for t in range(tokens):
        hits = [(expert == ids_ref[t, j]).astype(I32) for j in range(picks)]
        named = sum(hits)
        first = named * (count == part).astype(I32)
        third = named * (count == 2).astype(I32)
        out.append((hits, first, third))
        count = count + named
    return out, side, part


def pack_body(block, here_ref, ids_ref, tok_ref, o_ref):
    rows, width = o_ref.shape
    half = block // 2
    low = width - half
    routes, side, part = routing(ids_ref, rows)
    start = pl.multiple_of(here_ref[0] * block, 128)
    tok = tok_ref[:, pl.ds(start, block)].astype(F32)
    main = jnp.zeros((rows, half), F32)
    tail = jnp.zeros((rows, low), F32)
    for t, (_, first, third) in enumerate(routes):
        for p in range(2):
            piece = tok[t : t + 1, p * half : (p + 1) * half]
            here = (side == p).astype(I32)
            main = main + (first * here).astype(F32) * piece
            rest = piece[:, low:]
            if 2 * low > half:
                rest = jnp.concatenate([rest, jnp.zeros((1, 2 * low - half), F32)], axis=1)
            third_here = third * here
            tail = tail + (third_here * (1 - part)).astype(F32) * piece[:, :low]
            tail = tail + (third_here * part).astype(F32) * rest
    o_ref[:, :half] = main.astype(BF)
    o_ref[:, half:] = tail.astype(BF)


def packed_of(here, ids, tokens, owners, block):
    half = block // 2
    width = half + split_of(half)

    def kernel(*refs):
        pack_body(block, *refs)

    return pl.pallas_call(
        kernel,
        out_shape=jax.ShapeDtypeStruct((2 * owners, width), BF),
        in_specs=[SM, SM, VM],
        out_specs=VM,
        compiler_params=params(4),
        name="pack",
    )(here, ids, tokens)


def mix_kernel(ids_ref, code_ref, x_ref, o_ref):
    rows, width = x_ref.shape
    half = o_ref.shape[1] // 2
    low = width - half
    routes, side, part = routing(ids_ref, rows)
    x = x_ref[...].astype(F32)
    for t, (hits, first, third) in enumerate(routes):
        code = sum(hit * code_ref[t, j] for j, hit in enumerate(hits))
        weight = code.astype(F32) / 64.0
        for p in range(2):
            here = (side == p).astype(I32)

            def total(chosen, lo, hi):
                scaled = (chosen * here).astype(F32) * weight * x[:, lo:hi]
                return jnp.sum(scaled, axis=0, keepdims=True)

            main = total(first, 0, half)
            lower = total(third * (1 - part), half, width)
            upper = total(third * part, half, 2 * half - low)
            at = p * half
            o_ref[t : t + 1, at : at + low] = (main[:, :low] + lower).astype(BF)
            o_ref[t : t + 1, at + low : at + half] = (main[:, low:] + upper).astype(BF)


def mixed_of(ids, codes, x, block):
    return pl.pallas_call(
        mix_kernel,
        out_shape=jax.ShapeDtypeStruct((ids.shape[0], block), BF),
        in_specs=[SM, SM, VM],
        out_specs=VM,
        compiler_params=params(4),
        name="mix",
    )(ids, codes, x)


def fetch_kernel(g0, u0, d0, g1, u1, d1, g_ref, u_ref, d_ref, sems):
    copies = []
    for i, (src, dst) in enumerate(
        ((g0, g_ref), (u0, u_ref), (d0, d_ref), (g1, g_ref), (u1, u_ref), (d1, d_ref))
    ):
        units = src.shape[0]
        rows = pl.ds((i // 3) * units, units)
        copies.append(pltpu.make_async_copy(src, dst.at[rows], sems.at[i]))
    for copy in copies:
        copy.start()
    for copy in copies:
        copy.wait()


def fetched(own, other):
    units, features = own[0].shape
    shape = jax.ShapeDtypeStruct((2 * units, features), BF)
    return pl.pallas_call(
        fetch_kernel,
        out_shape=(shape,) * 3,
        in_specs=[ANY] * 6,
        out_specs=(VM,) * 3,
        scratch_shapes=[pltpu.SemaphoreType.DMA((6,))],
        cost_estimate=pl.CostEstimate(
            flops=12 * units * features * 256,
            bytes_accessed=24 * units * features,
            transcendentals=0,
        ),
        compiler_params=params(13),
        name="fetch",
    )(*(pltpu.with_memory_space_constraint(w, pltpu.MemorySpace.HBM) for w in own), *other)


def expert_kernel(here_ref, odd_ref, *refs):
    own_ref = refs[0]
    parts, owners, _, width = own_ref.shape
    pals, (g_ref, u_ref, d_ref, give_ref) = refs[1 : 1 + parts], refs[1 + parts : 5 + parts]
    keep_refs = refs[5 + parts :]
    rows = 2 * owners
    half = d_ref.shape[1] // (2 * parts)
    low = width - half
    units = g_ref.shape[0]
    odd, here = odd_ref[0], here_ref[0]

    def start(k, other):
        side = 1 - odd if other else odd
        return pl.multiple_of((2 * k + side) * half, 128)

    sums = [[jnp.zeros((2 * rows, units), F32) for _ in range(2)] for _ in range(2)]
    for i in range(2 * parts):
        if i < parts:
            x, at = own_ref[i], start(i, False)
        else:
            x, at = pals[i - parts][...], start(lax.rem(here + 2 * parts - i, parts), True)
        x = x.reshape(rows, width)
        lhs = (
            jnp.concatenate([x[:, :low], x[:, half:]], axis=0),
            jnp.concatenate([x[:, low:half], x[:, half : 2 * half - low]], axis=0),
        )
        for w, w_ref in enumerate((g_ref, u_ref)):
            for c, (lo, size) in enumerate(((0, low), (low, half - low))):
                cols = pl.ds(pl.multiple_of(at + lo, 128), size)
                sums[w][c] += lax.dot_general(
                    lhs[c], w_ref[:, cols], CONTRACT, preferred_element_type=F32
                )

    def joined(a, b):
        third = a[rows:] + pltpu.roll(b[rows:], rows - 1, 0)
        return jnp.concatenate([a[:rows] + b[:rows], third], axis=0)

    gate, up = joined(*sums[0]), joined(*sums[1])
    hidden = gate / (1.0 + jnp.exp(-gate)) * up
    third = hidden[rows:]
    even = lax.broadcasted_iota(I32, (rows, units), 0) % 2 == 0
    lower = jnp.where(even, third, 0.0)
    upper = jnp.where(even, 0.0, pltpu.roll(third, 1, 0))
    lhs = (
        jnp.concatenate([hidden[:rows], lower], axis=0).astype(BF),
        jnp.concatenate([hidden[:rows], upper], axis=0).astype(BF),
    )
    for other in (True, False):
        for k in range(parts):
            at = start(k if other else lax.rem(here + k, parts), other)
            o_ref = give_ref.at[k] if other else keep_refs[k]
            a = jnp.dot(lhs[0], d_ref[:, pl.ds(at, low)], preferred_element_type=F32)
            cols = pl.ds(pl.multiple_of(at + low, 128), half - low)
            b = jnp.dot(lhs[1], d_ref[:, cols], preferred_element_type=F32)
            o_ref[:, :low] = a[:rows].astype(BF)
            o_ref[:, low:half] = b[:rows].astype(BF)
            o_ref[:, half : 2 * half - low] = (a[rows:, : half - low] + b[rows:]).astype(BF)
            if 2 * low > half:
                o_ref[:, 2 * half - low :] = a[rows:, half - low :].astype(BF)


def experts_of(here, odd, own, pals, weights):
    parts, owners, _, width = own.shape
    units, features = weights[0].shape
    one = jax.ShapeDtypeStruct((2 * owners, width), BF)
    out = pl.pallas_call(
        expert_kernel,
        out_shape=(jax.ShapeDtypeStruct((parts, *one.shape), BF), *(one,) * parts),
        in_specs=[SM] * 2 + [VM] * (parts + 4),
        out_specs=(VM,) * (parts + 1),
        cost_estimate=pl.CostEstimate(
            flops=24 * owners * units * features,
            bytes_accessed=6 * units * features,
            transcendentals=4 * owners * units,
        ),
        compiler_params=params(24),
        name="experts",
    )(here, odd, own, *pals, *weights)
    return out[0], out[1:]


def shards(tokens, expert_ids, gate_codes, w_gate, w_up, w_down):
    rows, features = tokens.shape
    owners = lax.axis_size("expert")
    subs = lax.axis_size("sub")
    parts = lax.axis_size("tensor")
    experts = owners // 2
    assert min(rows, rows * expert_ids.shape[1] // experts + 1) == 3
    block = features // parts
    width = block // 2 + split_of(block // 2)
    here = lax.axis_index("tensor").reshape(1)
    odd = (lax.axis_index("expert") & 1).reshape(1)
    swap_sub = [(i, subs - 1 - i) for i in range(subs)]
    swap_pair = [(i, i ^ 1) for i in range(owners)]

    def turned(x, k):
        return lax.ppermute(x, "tensor", [(i, (i + k) % parts) for i in range(parts)])

    def across(x):
        return lax.all_to_all(x, "tensor", split_axis=0, concat_axis=0, tiled=True)

    def along(x):
        return lax.all_to_all(x, "expert", split_axis=0, concat_axis=0, tiled=True)

    own = (w_gate[0], w_up[0], w_down[0])
    other = [lax.ppermute(w, "sub", swap_sub) for w in own]
    weights = fetched(own, other)
    packed = packed_of(here, expert_ids, tokens, owners, block).reshape(owners, 2, width)
    arrived = along(packed)
    partner = lax.ppermute(arrived, "expert", swap_pair)
    spread = jnp.broadcast_to(arrived[None], (parts, *arrived.shape))
    spread = across(spread)
    pals = [partner] + [None] * (parts - 1)
    for k in ring_steps(parts):
        pals[k] = turned(partner, k)
    give, keep = experts_of(here, odd, spread, pals, weights)
    give = across(give)
    kept = [keep[0]]
    for k in ring_steps(parts):
        kept.append(turned(keep[k], k))
    give = jnp.sum(give.astype(F32), axis=0).astype(BF)
    taken = lax.ppermute(give, "expert", swap_pair)
    both = sum(x.astype(F32) for x in kept) + taken.astype(F32)
    both = both.astype(BF).reshape(owners, 2, width)
    back = along(both).reshape(2 * owners, width)
    return mixed_of(expert_ids, gate_codes, back, block)


def ring_steps(parts):
    return sorted(range(1, parts), key=lambda k: min(k, parts - k))


def solution(mesh):
    spread = P(("group", "expert", "sub"), None)
    weights = P("expert", ("tensor", "sub"), None)
    return jax.shard_map(
        shards,
        mesh=mesh,
        in_specs=(spread, spread, spread, weights, weights, weights),
        out_specs=P(("group", "expert", "sub"), "tensor"),
        check_vma=False,
    )
```

```python
import jax
import jax.numpy as jnp
from jax import lax
from jax.experimental import pallas as pl
from jax.experimental.pallas import tpu as pltpu
from jax.sharding import PartitionSpec as P

BF = jnp.bfloat16
F32 = jnp.float32
I32 = jnp.int32
VM = pl.BlockSpec(memory_space=pltpu.VMEM)
SM = pl.BlockSpec(memory_space=pltpu.SMEM)
ANY = pl.BlockSpec(memory_space=pl.ANY)
CONTRACT = (((1,), (1,)), ((), ()))
MIB = 1024 * 1024


def params(mib):
    return pltpu.CompilerParams(vmem_limit_bytes=mib * MIB)


def split_of(half):
    return -(-half // 256) * 128


def routing(ids_ref, rows, axis):
    shape = (rows, 1) if axis == 0 else (1, rows)
    row = lax.broadcasted_iota(I32, shape, axis)
    expert, side, part = row // 4, (row // 2) % 2, row % 2
    tokens, picks = ids_ref.shape
    count = jnp.zeros(shape, I32)
    out = []
    for t in range(tokens):
        hits = [(expert == ids_ref[t, j]).astype(I32) for j in range(picks)]
        named = sum(hits)
        first = named * (count == part).astype(I32)
        third = named * (count == 2).astype(I32)
        out.append((hits, first, third))
        count = count + named
    return out, side, part


def pack_kernel(here_ref, ids_hbm, tok_hbm, o_ref, ids_ref, tok_ref, sems):
    owners, _, width = o_ref.shape
    rows = 2 * owners
    block = tok_ref.shape[1]
    half = block // 2
    low = width - half
    start = pl.multiple_of(here_ref[0] * block, 128)
    take_ids = pltpu.make_async_copy(ids_hbm, ids_ref, sems.at[0])
    take_tok = pltpu.make_async_copy(tok_hbm.at[:, pl.ds(start, block)], tok_ref, sems.at[1])
    take_ids.start()
    take_tok.start()
    take_ids.wait()
    routes, side, part = routing(ids_ref, rows, 0)
    take_tok.wait()
    tok = tok_ref[...].astype(F32)
    main = jnp.zeros((rows, half), F32)
    tail = jnp.zeros((rows, low), F32)
    for t, (_, first, third) in enumerate(routes):
        for p in range(2):
            piece = tok[t : t + 1, p * half : (p + 1) * half]
            here = (side == p).astype(I32)
            main = main + (first * here).astype(F32) * piece
            rest = piece[:, low:]
            if 2 * low > half:
                rest = jnp.concatenate([rest, jnp.zeros((1, 2 * low - half), F32)], axis=1)
            third_here = third * here
            tail = tail + (third_here * (1 - part)).astype(F32) * piece[:, :low]
            tail = tail + (third_here * part).astype(F32) * rest
    o_ref[:, :, :half] = main.astype(BF).reshape(owners, 2, half)
    o_ref[:, :, half:] = tail.astype(BF).reshape(owners, 2, low)


def in_hbm(x):
    return pltpu.with_memory_space_constraint(x, pltpu.MemorySpace.HBM)


def packed_of(here, ids, tokens, owners, block):
    half = block // 2
    width = half + split_of(half)
    return pl.pallas_call(
        pack_kernel,
        out_shape=jax.ShapeDtypeStruct((owners, 2, width), BF),
        in_specs=[SM, ANY, ANY],
        out_specs=VM,
        scratch_shapes=[
            pltpu.SMEM(ids.shape, I32),
            pltpu.VMEM((tokens.shape[0], block), BF),
            pltpu.SemaphoreType.DMA((2,)),
        ],
        compiler_params=params(4),
        name="pack",
    )(here, in_hbm(ids), in_hbm(tokens))


def mix_kernel(ids_ref, code_ref, x_ref, o_ref):
    owners, _, width = x_ref.shape
    rows = 2 * owners
    tokens = o_ref.shape[0]
    half = o_ref.shape[1] // 2
    low = width - half
    routes, side, part = routing(ids_ref, rows, 1)
    mains, lowers, uppers = [], [], []
    for p in range(2):
        for t, (hits, first, third) in enumerate(routes):
            code = sum(hit * code_ref[t, j] for j, hit in enumerate(hits))
            code = code * (side == p).astype(I32)
            mains.append(first * code)
            lowers.append(third * (1 - part) * code)
            uppers.append(third * part * code)
    weights = (jnp.concatenate(mains + lowers + uppers, axis=0).astype(F32) / 64.0).astype(BF)
    x = x_ref[...].reshape(rows, width)
    r = jnp.dot(weights, x, preferred_element_type=F32)
    n = 2 * tokens
    for p in range(2):
        at, main = p * half, r[p * tokens : (p + 1) * tokens, :half]
        lower = r[n + p * tokens : n + (p + 1) * tokens, half:]
        upper = r[2 * n + p * tokens : 2 * n + (p + 1) * tokens, half : 2 * half - low]
        o_ref[:, at : at + low] = (main[:, :low] + lower).astype(BF)
        o_ref[:, at + low : at + half] = (main[:, low:] + upper).astype(BF)


def mixed_of(ids, codes, x, block):
    return pl.pallas_call(
        mix_kernel,
        out_shape=jax.ShapeDtypeStruct((ids.shape[0], block), BF),
        in_specs=[SM, SM, VM],
        out_specs=VM,
        compiler_params=params(4),
        name="mix",
    )(ids, codes, x)


def start_of(here, odd, parts, half, k, other, turned):
    side = 1 - odd if other else odd
    k = lax.rem(here + k, parts) if turned else k
    return pl.multiple_of((2 * k + side) * half, 128)


def halves_of(x, half):
    width = x.shape[-1]
    low = width - half
    x = x.reshape(-1, width)
    return (
        (0, low, jnp.concatenate([x[:, :low], x[:, half:]], axis=0)),
        (low, half - low, jnp.concatenate([x[:, low:half], x[:, half : 2 * half - low]], axis=0)),
    )


def add_in(sums, x, at, w_ref, half):
    return [
        total
        + lax.dot_general(
            lhs,
            w_ref[:, pl.ds(pl.multiple_of(at + lo, 128), size)],
            CONTRACT,
            preferred_element_type=F32,
        )
        for total, (lo, size, lhs) in zip(sums, halves_of(x, half))
    ]


def own_kernel(here_ref, odd_ref, own_ref, g0, u0, d0, g1, u1, d1, g_ref, u_ref, d_ref, s_ref, sems):
    parts, _, _, _ = own_ref.shape
    half = d_ref.shape[1] // (2 * parts)
    copies = []
    for i, (pair, dst) in enumerate((((g0, g1), g_ref), ((u0, u1), u_ref), ((d0, d1), d_ref))):
        for c, src in enumerate(pair):
            units = src.shape[0]
            rows = pl.ds(c * units, units)
            copies.append(pltpu.make_async_copy(src, dst.at[rows], sems.at[2 * i + c]))
    for copy in copies:
        copy.start()
    for i, w_ref in enumerate((g_ref, u_ref)):
        copies[2 * i].wait()
        copies[2 * i + 1].wait()
        sums = [jnp.zeros(s_ref.shape[1:], F32)] * 2
        for k in range(parts):
            at = start_of(here_ref[0], odd_ref[0], parts, half, k, False, False)
            sums = add_in(sums, own_ref[k], at, w_ref, half)
        s_ref[2 * i] = sums[0]
        s_ref[2 * i + 1] = sums[1]
    copies[4].wait()
    copies[5].wait()


def own_part(here, odd, own, mine, theirs):
    _, owners, _, _ = own.shape
    units, features = mine[0].shape
    shape = jax.ShapeDtypeStruct((2 * units, features), BF)
    return pl.pallas_call(
        own_kernel,
        out_shape=(shape,) * 3 + (jax.ShapeDtypeStruct((4, 4 * owners, 2 * units), F32),),
        in_specs=[SM, SM, VM] + [ANY] * 6,
        out_specs=(VM,) * 4,
        scratch_shapes=[pltpu.SemaphoreType.DMA((6,))],
        cost_estimate=pl.CostEstimate(
            flops=16 * owners * units * features,
            bytes_accessed=24 * units * features,
            transcendentals=0,
        ),
        compiler_params=params(16),
        name="ownpart",
    )(here, odd, own, *(in_hbm(w) for w in mine), *theirs)


def expert_kernel(here_ref, odd_ref, s_ref, *refs):
    parts = (len(refs) - 4) // 2
    pals, (g_ref, u_ref, d_ref, give_ref) = refs[:parts], refs[parts : parts + 4]
    keep_refs = refs[parts + 4 :]
    owners, _, width = pals[0].shape
    rows = 2 * owners
    half = d_ref.shape[1] // (2 * parts)
    low = width - half
    odd, here = odd_ref[0], here_ref[0]

    gates, ups = [s_ref[0], s_ref[1]], [s_ref[2], s_ref[3]]
    for i, x_ref in enumerate(pals):
        at = start_of(here, odd, parts, half, parts - i, True, True)
        gates = add_in(gates, x_ref[...], at, g_ref, half)
        ups = add_in(ups, x_ref[...], at, u_ref, half)

    def joined(a, b):
        third = a[rows:] + pltpu.roll(b[rows:], rows - 1, 0)
        return jnp.concatenate([a[:rows] + b[:rows], third], axis=0)

    gate, up = joined(*gates), joined(*ups)
    hidden = gate / (1.0 + jnp.exp(-gate)) * up
    third = hidden[rows:]
    even = lax.broadcasted_iota(I32, third.shape, 0) % 2 == 0
    lower = jnp.where(even, third, 0.0)
    upper = jnp.where(even, 0.0, pltpu.roll(third, 1, 0))
    lhs = (
        jnp.concatenate([hidden[:rows], lower], axis=0).astype(BF),
        jnp.concatenate([hidden[:rows], upper], axis=0).astype(BF),
    )
    for other in (True, False):
        for k in range(parts):
            at = start_of(here, odd, parts, half, k, other, not other)
            o_ref = give_ref.at[k] if other else keep_refs[k]
            a = jnp.dot(lhs[0], d_ref[:, pl.ds(at, low)], preferred_element_type=F32)
            cols = pl.ds(pl.multiple_of(at + low, 128), half - low)
            b = jnp.dot(lhs[1], d_ref[:, cols], preferred_element_type=F32)
            o_ref[:, :low] = a[:rows].astype(BF)
            o_ref[:, low:half] = b[:rows].astype(BF)
            o_ref[:, half : 2 * half - low] = (a[rows:, : half - low] + b[rows:]).astype(BF)
            if 2 * low > half:
                o_ref[:, 2 * half - low :] = a[rows:, half - low :].astype(BF)


def experts_of(here, odd, sums, pals, weights):
    parts = len(pals)
    owners, _, width = pals[0].shape
    units, features = weights[0].shape
    one = jax.ShapeDtypeStruct((2 * owners, width), BF)
    out = pl.pallas_call(
        expert_kernel,
        out_shape=(jax.ShapeDtypeStruct((parts, *one.shape), BF), *(one,) * parts),
        in_specs=[SM] * 2 + [VM] * (parts + 4),
        out_specs=(VM,) * (parts + 1),
        cost_estimate=pl.CostEstimate(
            flops=16 * owners * units * features,
            bytes_accessed=6 * units * features,
            transcendentals=4 * owners * units,
        ),
        compiler_params=params(24),
        name="experts",
    )(here, odd, sums, *pals, *weights)
    return out[0], out[1:]


def shards(tokens, expert_ids, gate_codes, w_gate, w_up, w_down):
    rows, features = tokens.shape
    owners = lax.axis_size("expert")
    subs = lax.axis_size("sub")
    parts = lax.axis_size("tensor")
    experts = owners // 2
    assert min(rows, rows * expert_ids.shape[1] // experts + 1) == 3
    block = features // parts
    here = lax.axis_index("tensor").reshape(1)
    odd = (lax.axis_index("expert") & 1).reshape(1)
    swap_sub = [(i, subs - 1 - i) for i in range(subs)]
    swap_pair = [(i, i ^ 1) for i in range(owners)]

    def turned(x, k):
        return lax.ppermute(x, "tensor", [(i, (i + k) % parts) for i in range(parts)])

    def across(x):
        return lax.all_to_all(x, "tensor", split_axis=0, concat_axis=0, tiled=True)

    def along(x):
        return lax.all_to_all(x, "expert", split_axis=0, concat_axis=0, tiled=True)

    own = (w_gate[0], w_up[0], w_down[0])
    other = [lax.ppermute(w, "sub", swap_sub) for w in own]
    packed = packed_of(here, expert_ids, tokens, owners, block)
    arrived = along(packed)
    partner = lax.ppermute(arrived, "expert", swap_pair)
    spread = jnp.broadcast_to(arrived[None], (parts, *arrived.shape))
    spread = across(spread)
    pals = [partner] + [None] * (parts - 1)
    for k in ring_steps(parts):
        pals[k] = turned(partner, k)
    *weights, sums = own_part(here, odd, spread, own, other)
    give, keep = experts_of(here, odd, sums, pals, weights)
    give = across(give)
    kept = [keep[0]]
    for k in ring_steps(parts):
        kept.append(turned(keep[k], k))
    give = jnp.sum(give.astype(F32), axis=0).astype(BF)
    taken = lax.ppermute(give, "expert", swap_pair)
    both = sum(x.astype(F32) for x in kept) + taken.astype(F32)
    both = both.astype(BF).reshape(arrived.shape)
    back = along(both)
    return mixed_of(expert_ids, gate_codes, back, block)


def ring_steps(parts):
    return sorted(range(1, parts), key=lambda k: min(k, parts - k))


def solution(mesh):
    spread = P(("group", "expert", "sub"), None)
    weights = P("expert", ("tensor", "sub"), None)
    return jax.shard_map(
        shards,
        mesh=mesh,
        in_specs=(spread, spread, spread, weights, weights, weights),
        out_specs=P(("group", "expert", "sub"), "tensor"),
        check_vma=False,
    )
```

```python
import jax
import jax.numpy as jnp
from jax import lax
from jax.experimental import pallas as pl
from jax.experimental.pallas import tpu as pltpu
from jax.sharding import PartitionSpec as P

BF = jnp.bfloat16
F32 = jnp.float32
I32 = jnp.int32
VM = pl.BlockSpec(memory_space=pltpu.VMEM)
SM = pl.BlockSpec(memory_space=pltpu.SMEM)
ANY = pl.BlockSpec(memory_space=pl.ANY)
CONTRACT = (((1,), (1,)), ((), ()))
MIB = 1024 * 1024


def params(mib):
    return pltpu.CompilerParams(vmem_limit_bytes=mib * MIB)


def split_of(half):
    return -(-half // 256) * 128


def routing(ids_ref, rows, axis):
    shape = (rows, 1) if axis == 0 else (1, rows)
    row = lax.broadcasted_iota(I32, shape, axis)
    expert, side, part = row // 4, (row // 2) % 2, row % 2
    tokens, picks = ids_ref.shape
    count = jnp.zeros(shape, I32)
    out = []
    for t in range(tokens):
        hits = [(expert == ids_ref[t, j]).astype(I32) for j in range(picks)]
        named = sum(hits)
        first = named * (count == part).astype(I32)
        third = named * (count == 2).astype(I32)
        out.append((hits, first, third))
        count = count + named
    return out, side, part


def pack_kernel(here_ref, ids_hbm, tok_hbm, o_ref, ids_ref, tok_ref, sems):
    owners, _, width = o_ref.shape
    rows = 2 * owners
    block = tok_ref.shape[1]
    half = block // 2
    low = width - half
    start = pl.multiple_of(here_ref[0] * block, 128)
    take_ids = pltpu.make_async_copy(ids_hbm, ids_ref, sems.at[0])
    take_tok = pltpu.make_async_copy(tok_hbm.at[:, pl.ds(start, block)], tok_ref, sems.at[1])
    take_ids.start()
    take_tok.start()
    take_ids.wait()
    routes, side, part = routing(ids_ref, rows, 0)
    take_tok.wait()
    tok = tok_ref[...].astype(F32)
    main = jnp.zeros((rows, half), F32)
    tail = jnp.zeros((rows, low), F32)
    for t, (_, first, third) in enumerate(routes):
        for p in range(2):
            piece = tok[t : t + 1, p * half : (p + 1) * half]
            here = (side == p).astype(I32)
            main = main + (first * here).astype(F32) * piece
            rest = piece[:, low:]
            if 2 * low > half:
                rest = jnp.concatenate([rest, jnp.zeros((1, 2 * low - half), F32)], axis=1)
            third_here = third * here
            tail = tail + (third_here * (1 - part)).astype(F32) * piece[:, :low]
            tail = tail + (third_here * part).astype(F32) * rest
    o_ref[:, :, :half] = main.astype(BF).reshape(owners, 2, half)
    o_ref[:, :, half:] = tail.astype(BF).reshape(owners, 2, low)


def in_hbm(x):
    return pltpu.with_memory_space_constraint(x, pltpu.MemorySpace.HBM)


def packed_of(here, ids, tokens, owners, block):
    half = block // 2
    width = half + split_of(half)
    return pl.pallas_call(
        pack_kernel,
        out_shape=jax.ShapeDtypeStruct((owners, 2, width), BF),
        in_specs=[SM, ANY, ANY],
        out_specs=VM,
        scratch_shapes=[
            pltpu.SMEM(ids.shape, I32),
            pltpu.VMEM((tokens.shape[0], block), BF),
            pltpu.SemaphoreType.DMA((2,)),
        ],
        compiler_params=params(4),
        name="pack",
    )(here, in_hbm(ids), in_hbm(tokens))


def mix_kernel(ids_ref, code_ref, x_ref, o_ref):
    owners, _, width = x_ref.shape
    rows = 2 * owners
    tokens = o_ref.shape[0]
    half = o_ref.shape[1] // 2
    low = width - half
    routes, side, part = routing(ids_ref, rows, 1)
    mains, lowers, uppers = [], [], []
    for p in range(2):
        for t, (hits, first, third) in enumerate(routes):
            code = sum(hit * code_ref[t, j] for j, hit in enumerate(hits))
            code = code * (side == p).astype(I32)
            mains.append(first * code)
            lowers.append(third * (1 - part) * code)
            uppers.append(third * part * code)
    weights = (jnp.concatenate(mains + lowers + uppers, axis=0).astype(F32) / 64.0).astype(BF)
    x = x_ref[...].reshape(rows, width)
    r = jnp.dot(weights, x, preferred_element_type=F32)
    n = 2 * tokens
    for p in range(2):
        at, main = p * half, r[p * tokens : (p + 1) * tokens, :half]
        lower = r[n + p * tokens : n + (p + 1) * tokens, half:]
        upper = r[2 * n + p * tokens : 2 * n + (p + 1) * tokens, half : 2 * half - low]
        o_ref[:, at : at + low] = (main[:, :low] + lower).astype(BF)
        o_ref[:, at + low : at + half] = (main[:, low:] + upper).astype(BF)


def mixed_of(ids, codes, x, block):
    return pl.pallas_call(
        mix_kernel,
        out_shape=jax.ShapeDtypeStruct((ids.shape[0], block), BF),
        in_specs=[SM, SM, VM],
        out_specs=VM,
        compiler_params=params(4),
        name="mix",
    )(ids, codes, x)


def start_of(here, odd, half, k, other, turned):
    side = 1 - odd if other else odd
    k = lax.bitwise_xor(here, jnp.int32(k)) if turned else k
    return pl.multiple_of((2 * k + side) * half, 128)


def halves_of(x, half):
    width = x.shape[-1]
    low = width - half
    x = x.reshape(-1, width)
    return (
        (0, low, jnp.concatenate([x[:, :low], x[:, half:]], axis=0)),
        (low, half - low, jnp.concatenate([x[:, low:half], x[:, half : 2 * half - low]], axis=0)),
    )


def add_in(sums, x, at, w_ref, half):
    return [
        total
        + lax.dot_general(
            lhs,
            w_ref[:, pl.ds(pl.multiple_of(at + lo, 128), size)],
            CONTRACT,
            preferred_element_type=F32,
        )
        for total, (lo, size, lhs) in zip(sums, halves_of(x, half))
    ]


def own_kernel(here_ref, odd_ref, *refs):
    parts = len(refs) - 11
    owns, (g0, u0, d0, g1, u1, d1, g_ref, u_ref, d_ref, s_ref, sems) = refs[:parts], refs[parts:]
    half = d_ref.shape[1] // (2 * parts)
    copies = []
    for i, (pair, dst) in enumerate((((g0, g1), g_ref), ((u0, u1), u_ref), ((d0, d1), d_ref))):
        for c, src in enumerate(pair):
            units = src.shape[0]
            rows = pl.ds(c * units, units)
            copies.append(pltpu.make_async_copy(src, dst.at[rows], sems.at[2 * i + c]))
    for copy in copies:
        copy.start()
    for i, w_ref in enumerate((g_ref, u_ref)):
        copies[2 * i].wait()
        copies[2 * i + 1].wait()
        sums = [jnp.zeros(s_ref.shape[1:], F32)] * 2
        for k in range(parts):
            at = start_of(here_ref[0], odd_ref[0], half, k, False, True)
            sums = add_in(sums, owns[k][...], at, w_ref, half)
        s_ref[2 * i] = sums[0]
        s_ref[2 * i + 1] = sums[1]
    copies[4].wait()
    copies[5].wait()


def own_part(here, odd, owns, mine, theirs):
    parts = len(owns)
    owners, _, _ = owns[0].shape
    units, features = mine[0].shape
    shape = jax.ShapeDtypeStruct((2 * units, features), BF)
    return pl.pallas_call(
        own_kernel,
        out_shape=(shape,) * 3 + (jax.ShapeDtypeStruct((4, 4 * owners, 2 * units), F32),),
        in_specs=[SM] * 2 + [VM] * parts + [ANY] * 6,
        out_specs=(VM,) * 4,
        scratch_shapes=[pltpu.SemaphoreType.DMA((6,))],
        cost_estimate=pl.CostEstimate(
            flops=16 * owners * units * features,
            bytes_accessed=24 * units * features,
            transcendentals=0,
        ),
        compiler_params=params(16),
        name="ownpart",
    )(here, odd, *owns, *(in_hbm(w) for w in mine), *theirs)


def expert_kernel(here_ref, odd_ref, s_ref, *refs):
    parts = (len(refs) - 4) // 2
    pals, (g_ref, u_ref, d_ref, give_ref) = refs[:parts], refs[parts : parts + 4]
    keep_refs = refs[parts + 4 :]
    owners, _, width = pals[0].shape
    rows = 2 * owners
    half = d_ref.shape[1] // (2 * parts)
    low = width - half
    odd, here = odd_ref[0], here_ref[0]

    gates, ups = [s_ref[0], s_ref[1]], [s_ref[2], s_ref[3]]
    for i, x_ref in enumerate(pals):
        at = start_of(here, odd, half, i, True, True)
        gates = add_in(gates, x_ref[...], at, g_ref, half)
        ups = add_in(ups, x_ref[...], at, u_ref, half)

    def joined(a, b):
        third = a[rows:] + pltpu.roll(b[rows:], rows - 1, 0)
        return jnp.concatenate([a[:rows] + b[:rows], third], axis=0)

    gate, up = joined(*gates), joined(*ups)
    hidden = gate / (1.0 + jnp.exp(-gate)) * up
    third = hidden[rows:]
    even = lax.broadcasted_iota(I32, third.shape, 0) % 2 == 0
    lower = jnp.where(even, third, 0.0)
    upper = jnp.where(even, 0.0, pltpu.roll(third, 1, 0))
    lhs = (
        jnp.concatenate([hidden[:rows], lower], axis=0).astype(BF),
        jnp.concatenate([hidden[:rows], upper], axis=0).astype(BF),
    )
    for other in (True, False):
        for k in range(parts):
            at = start_of(here, odd, half, k, other, not other)
            o_ref = give_ref.at[k] if other else keep_refs[k]
            a = jnp.dot(lhs[0], d_ref[:, pl.ds(at, low)], preferred_element_type=F32)
            cols = pl.ds(pl.multiple_of(at + low, 128), half - low)
            b = jnp.dot(lhs[1], d_ref[:, cols], preferred_element_type=F32)
            o_ref[:, :low] = a[:rows].astype(BF)
            o_ref[:, low:half] = b[:rows].astype(BF)
            o_ref[:, half : 2 * half - low] = (a[rows:, : half - low] + b[rows:]).astype(BF)
            if 2 * low > half:
                o_ref[:, 2 * half - low :] = a[rows:, half - low :].astype(BF)


def experts_of(here, odd, sums, pals, weights):
    parts = len(pals)
    owners, _, width = pals[0].shape
    units, features = weights[0].shape
    one = jax.ShapeDtypeStruct((2 * owners, width), BF)
    out = pl.pallas_call(
        expert_kernel,
        out_shape=(jax.ShapeDtypeStruct((parts, *one.shape), BF), *(one,) * parts),
        in_specs=[SM] * 2 + [VM] * (parts + 4),
        out_specs=(VM,) * (parts + 1),
        cost_estimate=pl.CostEstimate(
            flops=16 * owners * units * features,
            bytes_accessed=6 * units * features,
            transcendentals=4 * owners * units,
        ),
        compiler_params=params(24),
        name="experts",
    )(here, odd, sums, *pals, *weights)
    return out[0], out[1:]


def shards(tokens, expert_ids, gate_codes, w_gate, w_up, w_down):
    rows, features = tokens.shape
    owners = lax.axis_size("expert")
    subs = lax.axis_size("sub")
    parts = lax.axis_size("tensor")
    experts = owners // 2
    assert min(rows, rows * expert_ids.shape[1] // experts + 1) == 3
    block = features // parts
    here = lax.axis_index("tensor").reshape(1)
    odd = (lax.axis_index("expert") & 1).reshape(1)
    swap_sub = [(i, subs - 1 - i) for i in range(subs)]
    swap_pair = [(i, i ^ 1) for i in range(owners)]

    def swapped(x, k):
        return lax.ppermute(x, "tensor", [(i, i ^ k) for i in range(parts)])

    def across(x):
        return lax.all_to_all(x, "tensor", split_axis=0, concat_axis=0, tiled=True)

    def along(x):
        return lax.all_to_all(x, "expert", split_axis=0, concat_axis=0, tiled=True)

    own = (w_gate[0], w_up[0], w_down[0])
    other = [lax.ppermute(w, "sub", swap_sub) for w in own]
    packed = packed_of(here, expert_ids, tokens, owners, block)
    arrived = along(packed)
    partner = lax.ppermute(arrived, "expert", swap_pair)
    far, *near = swaps(parts)
    owns, pals = {0: arrived}, {0: partner}
    for k in (far, *near):
        owns[k] = swapped(arrived, k)
    for k in near:
        pals[k] = swapped(partner, k)
    pals[far] = lax.ppermute(owns[far], "expert", swap_pair)
    owns, pals = ([x[k] for k in range(parts)] for x in (owns, pals))
    *weights, sums = own_part(here, odd, owns, own, other)
    give, keep = experts_of(here, odd, sums, pals, weights)
    give = across(give)
    kept = [keep[0]]
    for k in (far, *near):
        kept.append(swapped(keep[k], k))
    give = jnp.sum(give.astype(F32), axis=0).astype(BF)
    taken = lax.ppermute(give, "expert", swap_pair)
    both = sum(x.astype(F32) for x in kept) + taken.astype(F32)
    both = both.astype(BF).reshape(arrived.shape)
    back = along(both)
    return mixed_of(expert_ids, gate_codes, back, block)


def swaps(parts):
    return [parts // 2, *(k for k in range(1, parts) if k != parts // 2)]


def solution(mesh):
    spread = P(("group", "expert", "sub"), None)
    weights = P("expert", ("tensor", "sub"), None)
    return jax.shard_map(
        shards,
        mesh=mesh,
        in_specs=(spread, spread, spread, weights, weights, weights),
        out_specs=P(("group", "expert", "sub"), "tensor"),
        check_vma=False,
    )
```

```python
import jax
import jax.numpy as jnp
from jax import lax
from jax.experimental import pallas as pl
from jax.experimental.pallas import tpu as pltpu
from jax.sharding import PartitionSpec as P

BF = jnp.bfloat16
F32 = jnp.float32
I32 = jnp.int32
VM = pl.BlockSpec(memory_space=pltpu.VMEM)
SM = pl.BlockSpec(memory_space=pltpu.SMEM)
ANY = pl.BlockSpec(memory_space=pl.ANY)
CONTRACT = (((1,), (1,)), ((), ()))
MIB = 1024 * 1024


def params(mib):
    return pltpu.CompilerParams(vmem_limit_bytes=mib * MIB)


def split_of(half):
    return -(-half // 256) * 128


def routing(ids_ref, rows, axis):
    shape = (rows, 1) if axis == 0 else (1, rows)
    row = lax.broadcasted_iota(I32, shape, axis)
    expert, side, part = row // 4, (row // 2) % 2, row % 2
    tokens, picks = ids_ref.shape
    count = jnp.zeros(shape, I32)
    out = []
    for t in range(tokens):
        hits = [(expert == ids_ref[t, j]).astype(I32) for j in range(picks)]
        named = sum(hits)
        first = named * (count == part).astype(I32)
        third = named * (count == 2).astype(I32)
        out.append((hits, first, third))
        count = count + named
    return out, side, part


def pack_kernel(here_ref, ids_hbm, tok_hbm, o_ref, ids_ref, tok_ref, sems):
    owners, _, width = o_ref.shape
    rows = 2 * owners
    block = tok_ref.shape[1]
    half = block // 2
    low = width - half
    start = pl.multiple_of(here_ref[0] * block, 128)
    take_ids = pltpu.make_async_copy(ids_hbm, ids_ref, sems.at[0])
    take_tok = pltpu.make_async_copy(tok_hbm.at[:, pl.ds(start, block)], tok_ref, sems.at[1])
    take_ids.start()
    take_tok.start()
    take_ids.wait()
    routes, side, part = routing(ids_ref, rows, 0)
    take_tok.wait()
    tok = tok_ref[...].astype(F32)
    main = jnp.zeros((rows, half), F32)
    tail = jnp.zeros((rows, low), F32)
    for t, (_, first, third) in enumerate(routes):
        for p in range(2):
            piece = tok[t : t + 1, p * half : (p + 1) * half]
            here = (side == p).astype(I32)
            main = main + (first * here).astype(F32) * piece
            rest = piece[:, low:]
            if 2 * low > half:
                rest = jnp.concatenate([rest, jnp.zeros((1, 2 * low - half), F32)], axis=1)
            third_here = third * here
            tail = tail + (third_here * (1 - part)).astype(F32) * piece[:, :low]
            tail = tail + (third_here * part).astype(F32) * rest
    o_ref[:, :, :half] = main.astype(BF).reshape(owners, 2, half)
    o_ref[:, :, half:] = tail.astype(BF).reshape(owners, 2, low)


def in_hbm(x):
    return pltpu.with_memory_space_constraint(x, pltpu.MemorySpace.HBM)


def packed_of(here, ids, tokens, owners, block):
    half = block // 2
    width = half + split_of(half)
    return pl.pallas_call(
        pack_kernel,
        out_shape=jax.ShapeDtypeStruct((owners, 2, width), BF),
        in_specs=[SM, ANY, ANY],
        out_specs=VM,
        scratch_shapes=[
            pltpu.SMEM(ids.shape, I32),
            pltpu.VMEM((tokens.shape[0], block), BF),
            pltpu.SemaphoreType.DMA((2,)),
        ],
        compiler_params=params(4),
        name="pack",
    )(here, in_hbm(ids), in_hbm(tokens))


def mix_kernel(ids_ref, code_ref, x_ref, o_ref):
    owners, _, width = x_ref.shape
    rows = 2 * owners
    tokens = o_ref.shape[0]
    half = o_ref.shape[1] // 2
    low = width - half
    routes, side, part = routing(ids_ref, rows, 1)
    mains, lowers, uppers = [], [], []
    for p in range(2):
        for t, (hits, first, third) in enumerate(routes):
            code = sum(hit * code_ref[t, j] for j, hit in enumerate(hits))
            code = code * (side == p).astype(I32)
            mains.append(first * code)
            lowers.append(third * (1 - part) * code)
            uppers.append(third * part * code)
    weights = (jnp.concatenate(mains + lowers + uppers, axis=0).astype(F32) / 64.0).astype(BF)
    x = x_ref[...].reshape(rows, width)
    r = jnp.dot(weights, x, preferred_element_type=F32)
    n = 2 * tokens
    for p in range(2):
        at, main = p * half, r[p * tokens : (p + 1) * tokens, :half]
        lower = r[n + p * tokens : n + (p + 1) * tokens, half:]
        upper = r[2 * n + p * tokens : 2 * n + (p + 1) * tokens, half : 2 * half - low]
        o_ref[:, at : at + low] = (main[:, :low] + lower).astype(BF)
        o_ref[:, at + low : at + half] = (main[:, low:] + upper).astype(BF)


def mixed_of(ids, codes, x, block):
    return pl.pallas_call(
        mix_kernel,
        out_shape=jax.ShapeDtypeStruct((ids.shape[0], block), BF),
        in_specs=[SM, SM, VM],
        out_specs=VM,
        compiler_params=params(4),
        name="mix",
    )(ids, codes, x)


def start_of(here, odd, half, k, other, turned):
    side = 1 - odd if other else odd
    k = lax.bitwise_xor(here, jnp.int32(k)) if turned else k
    return pl.multiple_of((2 * k + side) * half, 128)


def halves_of(x, half):
    width = x.shape[-1]
    low = width - half
    x = x.reshape(-1, width)
    return (
        (0, low, jnp.concatenate([x[:, :low], x[:, half:]], axis=0)),
        (low, half - low, jnp.concatenate([x[:, low:half], x[:, half : 2 * half - low]], axis=0)),
    )


def add_in(sums, x, at, w_ref, half):
    return [
        total
        + lax.dot_general(
            lhs,
            w_ref[:, pl.ds(pl.multiple_of(at + lo, 128), size)],
            CONTRACT,
            preferred_element_type=F32,
        )
        for total, (lo, size, lhs) in zip(sums, halves_of(x, half))
    ]


def own_kernel(here_ref, odd_ref, *refs):
    own_ref, g0, u0, d0, g1, u1, d1, g_ref, u_ref, d_ref, s_ref, sems = refs
    parts = own_ref.shape[0]
    half = d_ref.shape[1] // (2 * parts)
    copies = []
    for i, (pair, dst) in enumerate((((g0, g1), g_ref), ((u0, u1), u_ref), ((d0, d1), d_ref))):
        for c, src in enumerate(pair):
            units = src.shape[0]
            rows = pl.ds(c * units, units)
            copies.append(pltpu.make_async_copy(src, dst.at[rows], sems.at[2 * i + c]))
    for copy in copies:
        copy.start()
    for i, w_ref in enumerate((g_ref, u_ref)):
        copies[2 * i].wait()
        copies[2 * i + 1].wait()
        sums = [jnp.zeros(s_ref.shape[1:], F32)] * 2
        for k in range(parts):
            at = start_of(here_ref[0], odd_ref[0], half, k, False, False)
            sums = add_in(sums, own_ref[k], at, w_ref, half)
        s_ref[2 * i] = sums[0]
        s_ref[2 * i + 1] = sums[1]
    copies[4].wait()
    copies[5].wait()


def own_part(here, odd, own, mine, theirs):
    _, owners, _, _ = own.shape
    units, features = mine[0].shape
    shape = jax.ShapeDtypeStruct((2 * units, features), BF)
    return pl.pallas_call(
        own_kernel,
        out_shape=(shape,) * 3 + (jax.ShapeDtypeStruct((4, 4 * owners, 2 * units), F32),),
        in_specs=[SM, SM, VM] + [ANY] * 6,
        out_specs=(VM,) * 4,
        scratch_shapes=[pltpu.SemaphoreType.DMA((6,))],
        cost_estimate=pl.CostEstimate(
            flops=16 * owners * units * features,
            bytes_accessed=24 * units * features,
            transcendentals=0,
        ),
        compiler_params=params(16),
        name="ownpart",
    )(here, odd, own, *(in_hbm(w) for w in mine), *theirs)


def expert_kernel(here_ref, odd_ref, s_ref, *refs):
    parts = (len(refs) - 4) // 2
    pals, (g_ref, u_ref, d_ref, keep_ref) = refs[:parts], refs[parts : parts + 4]
    give_refs = refs[parts + 4 :]
    owners, _, width = pals[0].shape
    rows = 2 * owners
    half = d_ref.shape[1] // (2 * parts)
    low = width - half
    odd, here = odd_ref[0], here_ref[0]

    gates, ups = [s_ref[0], s_ref[1]], [s_ref[2], s_ref[3]]
    for i, x_ref in enumerate(pals):
        at = start_of(here, odd, half, i, True, True)
        gates = add_in(gates, x_ref[...], at, g_ref, half)
        ups = add_in(ups, x_ref[...], at, u_ref, half)

    def joined(a, b):
        third = a[rows:] + pltpu.roll(b[rows:], rows - 1, 0)
        return jnp.concatenate([a[:rows] + b[:rows], third], axis=0)

    gate, up = joined(*gates), joined(*ups)
    hidden = gate / (1.0 + jnp.exp(-gate)) * up
    third = hidden[rows:]
    even = lax.broadcasted_iota(I32, third.shape, 0) % 2 == 0
    lower = jnp.where(even, third, 0.0)
    upper = jnp.where(even, 0.0, pltpu.roll(third, 1, 0))
    lhs = (
        jnp.concatenate([hidden[:rows], lower], axis=0).astype(BF),
        jnp.concatenate([hidden[:rows], upper], axis=0).astype(BF),
    )
    for other in (True, False):
        for k in range(parts):
            at = start_of(here, odd, half, k, other, other)
            o_ref = give_refs[k] if other else keep_ref.at[k]
            a = jnp.dot(lhs[0], d_ref[:, pl.ds(at, low)], preferred_element_type=F32)
            cols = pl.ds(pl.multiple_of(at + low, 128), half - low)
            b = jnp.dot(lhs[1], d_ref[:, cols], preferred_element_type=F32)
            o_ref[:, :low] = a[:rows].astype(BF)
            o_ref[:, low:half] = b[:rows].astype(BF)
            o_ref[:, half : 2 * half - low] = (a[rows:, : half - low] + b[rows:]).astype(BF)
            if 2 * low > half:
                o_ref[:, 2 * half - low :] = a[rows:, half - low :].astype(BF)


def experts_of(here, odd, sums, pals, weights):
    parts = len(pals)
    owners, _, width = pals[0].shape
    units, features = weights[0].shape
    one = jax.ShapeDtypeStruct((2 * owners, width), BF)
    out = pl.pallas_call(
        expert_kernel,
        out_shape=(jax.ShapeDtypeStruct((parts, *one.shape), BF), *(one,) * parts),
        in_specs=[SM] * 2 + [VM] * (parts + 4),
        out_specs=(VM,) * (parts + 1),
        cost_estimate=pl.CostEstimate(
            flops=16 * owners * units * features,
            bytes_accessed=6 * units * features,
            transcendentals=4 * owners * units,
        ),
        compiler_params=params(24),
        name="experts",
    )(here, odd, sums, *pals, *weights)
    return out[0], out[1:]


def shards(tokens, expert_ids, gate_codes, w_gate, w_up, w_down):
    rows, features = tokens.shape
    owners = lax.axis_size("expert")
    subs = lax.axis_size("sub")
    parts = lax.axis_size("tensor")
    experts = owners // 2
    assert min(rows, rows * expert_ids.shape[1] // experts + 1) == 3
    block = features // parts
    here = lax.axis_index("tensor").reshape(1)
    odd = (lax.axis_index("expert") & 1).reshape(1)
    swap_sub = [(i, subs - 1 - i) for i in range(subs)]
    swap_pair = [(i, i ^ 1) for i in range(owners)]

    def swapped(x, k):
        return lax.ppermute(x, "tensor", [(i, i ^ k) for i in range(parts)])

    def across(x):
        return lax.all_to_all(x, "tensor", split_axis=0, concat_axis=0, tiled=True)

    def along(x):
        return lax.all_to_all(x, "expert", split_axis=0, concat_axis=0, tiled=True)

    own = (w_gate[0], w_up[0], w_down[0])
    other = [lax.ppermute(w, "sub", swap_sub) for w in own]
    packed = packed_of(here, expert_ids, tokens, owners, block)
    arrived = along(packed)
    partner = lax.ppermute(arrived, "expert", swap_pair)
    spread = jnp.broadcast_to(arrived[None], (parts, *arrived.shape))
    spread = across(spread)
    pals = [partner] + [None] * (parts - 1)
    for k in swaps(parts):
        pals[k] = swapped(partner, k)
    *weights, sums = own_part(here, odd, spread, own, other)
    keep, give = experts_of(here, odd, sums, pals, weights)
    given = [give[0]]
    for k in swaps(parts):
        given.append(swapped(give[k], k))
    keep = across(keep)
    give = sum(x.astype(F32) for x in given).astype(BF)
    taken = lax.ppermute(give, "expert", swap_pair)
    both = jnp.sum(keep.astype(F32), axis=0) + taken.astype(F32)
    both = both.astype(BF).reshape(arrived.shape)
    back = along(both)
    return mixed_of(expert_ids, gate_codes, back, block)


def swaps(parts):
    return sorted(range(1, parts), key=lambda k: k == parts // 2)


def solution(mesh):
    spread = P(("group", "expert", "sub"), None)
    weights = P("expert", ("tensor", "sub"), None)
    return jax.shard_map(
        shards,
        mesh=mesh,
        in_specs=(spread, spread, spread, weights, weights, weights),
        out_specs=P(("group", "expert", "sub"), "tensor"),
        check_vma=False,
    )
```

```python
import jax
import jax.numpy as jnp
from jax import lax
from jax.experimental import pallas as pl
from jax.experimental.pallas import tpu as pltpu
from jax.sharding import PartitionSpec as P

BF = jnp.bfloat16
F32 = jnp.float32
I32 = jnp.int32
VM = pl.BlockSpec(memory_space=pltpu.VMEM)
SM = pl.BlockSpec(memory_space=pltpu.SMEM)
ANY = pl.BlockSpec(memory_space=pl.ANY)
CONTRACT = (((1,), (1,)), ((), ()))
MIB = 1024 * 1024


def params(mib):
    return pltpu.CompilerParams(vmem_limit_bytes=mib * MIB)


def split_of(half):
    return -(-half // 256) * 128


def routing(ids_ref, rows, axis):
    shape = (rows, 1) if axis == 0 else (1, rows)
    row = lax.broadcasted_iota(I32, shape, axis)
    expert, side, part = row // 4, (row // 2) % 2, row % 2
    tokens, picks = ids_ref.shape
    count = jnp.zeros(shape, I32)
    out = []
    for t in range(tokens):
        hits = [(expert == ids_ref[t, j]).astype(I32) for j in range(picks)]
        named = sum(hits)
        first = named * (count == part).astype(I32)
        third = named * (count == 2).astype(I32)
        out.append((hits, first, third))
        count = count + named
    return out, side, part


def pack_kernel(here_ref, ids_hbm, tok_hbm, o_ref, ids_ref, tok_ref, sems):
    owners, _, width = o_ref.shape
    rows = 2 * owners
    block = tok_ref.shape[1]
    half = block // 2
    low = width - half
    start = pl.multiple_of(here_ref[0] * block, 128)
    take_ids = pltpu.make_async_copy(ids_hbm, ids_ref, sems.at[0])
    take_tok = pltpu.make_async_copy(tok_hbm.at[:, pl.ds(start, block)], tok_ref, sems.at[1])
    take_ids.start()
    take_tok.start()
    take_ids.wait()
    routes, side, part = routing(ids_ref, rows, 0)
    take_tok.wait()
    tok = tok_ref[...].astype(F32)
    main = jnp.zeros((rows, half), F32)
    tail = jnp.zeros((rows, low), F32)
    for t, (_, first, third) in enumerate(routes):
        for p in range(2):
            piece = tok[t : t + 1, p * half : (p + 1) * half]
            here = (side == p).astype(I32)
            main = main + (first * here).astype(F32) * piece
            rest = piece[:, low:]
            if 2 * low > half:
                rest = jnp.concatenate([rest, jnp.zeros((1, 2 * low - half), F32)], axis=1)
            third_here = third * here
            tail = tail + (third_here * (1 - part)).astype(F32) * piece[:, :low]
            tail = tail + (third_here * part).astype(F32) * rest
    o_ref[:, :, :half] = main.astype(BF).reshape(owners, 2, half)
    o_ref[:, :, half:] = tail.astype(BF).reshape(owners, 2, low)


def in_hbm(x):
    return pltpu.with_memory_space_constraint(x, pltpu.MemorySpace.HBM)


def packed_of(here, ids, tokens, owners, block):
    half = block // 2
    width = half + split_of(half)
    return pl.pallas_call(
        pack_kernel,
        out_shape=jax.ShapeDtypeStruct((owners, 2, width), BF),
        in_specs=[SM, ANY, ANY],
        out_specs=VM,
        scratch_shapes=[
            pltpu.SMEM(ids.shape, I32),
            pltpu.VMEM((tokens.shape[0], block), BF),
            pltpu.SemaphoreType.DMA((2,)),
        ],
        compiler_params=params(4),
        name="pack",
    )(here, in_hbm(ids), in_hbm(tokens))


def route_kernel(ids_ref, code_ref, w_ref):
    routes, side, part = routing(ids_ref, w_ref.shape[1], 1)
    mains, lowers, uppers = [], [], []
    for p in range(2):
        for t, (hits, first, third) in enumerate(routes):
            code = sum(hit * code_ref[t, j] for j, hit in enumerate(hits))
            code = code * (side == p).astype(I32)
            mains.append(first * code)
            lowers.append(third * (1 - part) * code)
            uppers.append(third * part * code)
    weights = jnp.concatenate(mains + lowers + uppers, axis=0).astype(F32) / 64.0
    w_ref[...] = weights.astype(BF)


def route_of(ids, codes, owners):
    return pl.pallas_call(
        route_kernel,
        out_shape=jax.ShapeDtypeStruct((6 * ids.shape[0], 2 * owners), BF),
        in_specs=[SM, SM],
        out_specs=VM,
        compiler_params=params(4),
        name="route",
    )(ids, codes)


def mix_kernel(w_ref, x_ref, o_ref):
    owners, _, width = x_ref.shape
    tokens = o_ref.shape[0]
    half = o_ref.shape[1] // 2
    low = width - half
    x = x_ref[...].reshape(2 * owners, width)
    r = jnp.dot(w_ref[...], x, preferred_element_type=F32)
    n = 2 * tokens
    for p in range(2):
        at, main = p * half, r[p * tokens : (p + 1) * tokens, :half]
        lower = r[n + p * tokens : n + (p + 1) * tokens, half:]
        upper = r[2 * n + p * tokens : 2 * n + (p + 1) * tokens, half : 2 * half - low]
        o_ref[:, at : at + low] = (main[:, :low] + lower).astype(BF)
        o_ref[:, at + low : at + half] = (main[:, low:] + upper).astype(BF)


def mixed_of(weights, x, tokens, block):
    return pl.pallas_call(
        mix_kernel,
        out_shape=jax.ShapeDtypeStruct((tokens, block), BF),
        in_specs=[VM, VM],
        out_specs=VM,
        compiler_params=params(4),
        name="mix",
    )(weights, x)


def start_of(here, odd, half, k, other, turned):
    side = 1 - odd if other else odd
    k = lax.bitwise_xor(here, jnp.int32(k)) if turned else k
    return pl.multiple_of((2 * k + side) * half, 128)


def halves_of(x, half):
    width = x.shape[-1]
    low = width - half
    x = x.reshape(-1, width)
    return (
        (0, low, jnp.concatenate([x[:, :low], x[:, half:]], axis=0)),
        (low, half - low, jnp.concatenate([x[:, low:half], x[:, half : 2 * half - low]], axis=0)),
    )


def add_in(sums, x, at, w_ref, half):
    return [
        total
        + lax.dot_general(
            lhs,
            w_ref[:, pl.ds(pl.multiple_of(at + lo, 128), size)],
            CONTRACT,
            preferred_element_type=F32,
        )
        for total, (lo, size, lhs) in zip(sums, halves_of(x, half))
    ]


def own_kernel(here_ref, odd_ref, *refs):
    own_ref, g0, u0, d0, g1, u1, d1, g_ref, u_ref, d_ref, s_ref, sems = refs
    parts = own_ref.shape[0]
    half = d_ref.shape[1] // (2 * parts)
    copies = []
    for i, (pair, dst) in enumerate((((g0, g1), g_ref), ((u0, u1), u_ref), ((d0, d1), d_ref))):
        for c, src in enumerate(pair):
            units = src.shape[0]
            rows = pl.ds(c * units, units)
            copies.append(pltpu.make_async_copy(src, dst.at[rows], sems.at[2 * i + c]))
    for copy in copies:
        copy.start()
    for i, w_ref in enumerate((g_ref, u_ref)):
        copies[2 * i].wait()
        copies[2 * i + 1].wait()
        sums = [jnp.zeros(s_ref.shape[1:], F32)] * 2
        for k in range(parts):
            at = start_of(here_ref[0], odd_ref[0], half, k, False, False)
            sums = add_in(sums, own_ref[k], at, w_ref, half)
        s_ref[2 * i] = sums[0]
        s_ref[2 * i + 1] = sums[1]
    copies[4].wait()
    copies[5].wait()


def own_part(here, odd, own, mine, theirs):
    _, owners, _, _ = own.shape
    units, features = mine[0].shape
    shape = jax.ShapeDtypeStruct((2 * units, features), BF)
    return pl.pallas_call(
        own_kernel,
        out_shape=(shape,) * 3 + (jax.ShapeDtypeStruct((4, 4 * owners, 2 * units), F32),),
        in_specs=[SM, SM, VM] + [ANY] * 6,
        out_specs=(VM,) * 4,
        scratch_shapes=[pltpu.SemaphoreType.DMA((6,))],
        cost_estimate=pl.CostEstimate(
            flops=16 * owners * units * features,
            bytes_accessed=24 * units * features,
            transcendentals=0,
        ),
        compiler_params=params(16),
        name="ownpart",
    )(here, odd, own, *(in_hbm(w) for w in mine), *theirs)


def expert_kernel(here_ref, odd_ref, s_ref, *refs):
    parts = (len(refs) - 5) // 2
    pals, (g_ref, u_ref, d_ref, a_ref, b_ref) = refs[:parts], refs[parts : parts + 5]
    give_refs = refs[parts + 5 :]
    owners = pals[0].shape[0]
    rows = 2 * owners
    half = d_ref.shape[1] // (2 * parts)
    odd, here = odd_ref[0], here_ref[0]

    gates, ups = [s_ref[0], s_ref[1]], [s_ref[2], s_ref[3]]
    for i, x_ref in enumerate(pals):
        at = start_of(here, odd, half, i, True, True)
        gates = add_in(gates, x_ref[...], at, g_ref, half)
        ups = add_in(ups, x_ref[...], at, u_ref, half)

    def joined(a, b):
        third = a[rows:] + pltpu.roll(b[rows:], rows - 1, 0)
        return jnp.concatenate([a[:rows] + b[:rows], third], axis=0)

    gate, up = joined(*gates), joined(*ups)
    hidden = gate / (1.0 + jnp.exp(-gate)) * up
    third = hidden[rows:]
    even = lax.broadcasted_iota(I32, third.shape, 0) % 2 == 0
    lower = jnp.where(even, third, 0.0)
    upper = jnp.where(even, 0.0, pltpu.roll(third, 1, 0))
    a_ref[...] = jnp.concatenate([hidden[:rows], lower], axis=0).astype(BF)
    b_ref[...] = jnp.concatenate([hidden[:rows], upper], axis=0).astype(BF)
    for k in range(parts):
        at = start_of(here, odd, half, k, True, True)
        down_into(give_refs[k], a_ref[...], b_ref[...], d_ref, at, half)


def down_into(o_ref, first, second, d_ref, at, half):
    rows, width = o_ref.shape
    low = width - half
    a = jnp.dot(first, d_ref[:, pl.ds(at, low)], preferred_element_type=F32)
    cols = pl.ds(pl.multiple_of(at + low, 128), half - low)
    b = jnp.dot(second, d_ref[:, cols], preferred_element_type=F32)
    o_ref[:, :low] = a[:rows].astype(BF)
    o_ref[:, low:half] = b[:rows].astype(BF)
    o_ref[:, half : 2 * half - low] = (a[rows:, : half - low] + b[rows:]).astype(BF)
    if 2 * low > half:
        o_ref[:, 2 * half - low :] = a[rows:, half - low :].astype(BF)


def keep_kernel(odd_ref, a_ref, b_ref, d_ref, o_ref):
    parts = o_ref.shape[0]
    half = d_ref.shape[1] // (2 * parts)
    for k in range(parts):
        at = start_of(0, odd_ref[0], half, k, False, False)
        down_into(o_ref.at[k], a_ref[...], b_ref[...], d_ref, at, half)


def experts_of(here, odd, sums, pals, weights):
    parts = len(pals)
    owners, _, width = pals[0].shape
    units, features = weights[0].shape
    lhs = jax.ShapeDtypeStruct((4 * owners, units), BF)
    one = jax.ShapeDtypeStruct((2 * owners, width), BF)
    a, b, *give = pl.pallas_call(
        expert_kernel,
        out_shape=(lhs, lhs, *(one,) * parts),
        in_specs=[SM] * 2 + [VM] * (parts + 4),
        out_specs=(VM,) * (parts + 2),
        cost_estimate=pl.CostEstimate(
            flops=12 * owners * units * features,
            bytes_accessed=6 * units * features,
            transcendentals=4 * owners * units,
        ),
        compiler_params=params(24),
        name="experts",
    )(here, odd, sums, *pals, *weights)
    return a, b, give


def keep_of(odd, a, b, down, parts, shape):
    return pl.pallas_call(
        keep_kernel,
        out_shape=jax.ShapeDtypeStruct((parts, *shape), BF),
        in_specs=[SM, VM, VM, VM],
        out_specs=VM,
        cost_estimate=pl.CostEstimate(
            flops=a.size * down.shape[1],
            bytes_accessed=2 * down.size,
            transcendentals=0,
        ),
        compiler_params=params(24),
        name="keepdown",
    )(odd, a, b, down)


def shards(tokens, expert_ids, gate_codes, w_gate, w_up, w_down):
    rows, features = tokens.shape
    owners = lax.axis_size("expert")
    subs = lax.axis_size("sub")
    parts = lax.axis_size("tensor")
    experts = owners // 2
    assert min(rows, rows * expert_ids.shape[1] // experts + 1) == 3
    block = features // parts
    here = lax.axis_index("tensor").reshape(1)
    odd = (lax.axis_index("expert") & 1).reshape(1)
    swap_sub = [(i, subs - 1 - i) for i in range(subs)]
    swap_pair = [(i, i ^ 1) for i in range(owners)]

    def swapped(x, k):
        return lax.ppermute(x, "tensor", [(i, i ^ k) for i in range(parts)])

    def across(x):
        return lax.all_to_all(x, "tensor", split_axis=0, concat_axis=0, tiled=True)

    def along(x):
        return lax.all_to_all(x, "expert", split_axis=0, concat_axis=0, tiled=True)

    own = (w_gate[0], w_up[0], w_down[0])
    other = [lax.ppermute(w, "sub", swap_sub) for w in own]
    packed = packed_of(here, expert_ids, tokens, owners, block)
    arrived = along(packed)
    route = route_of(expert_ids, gate_codes, owners)
    partner = lax.ppermute(arrived, "expert", swap_pair)
    spread = jnp.broadcast_to(arrived[None], (parts, *arrived.shape))
    spread = across(spread)
    pals = [partner] + [None] * (parts - 1)
    for k in swaps(parts):
        pals[k] = swapped(partner, k)
    *weights, sums = own_part(here, odd, spread, own, other)
    first, second, give = experts_of(here, odd, sums, pals, weights)
    given = [give[0]]
    for k in swaps(parts):
        given.append(swapped(give[k], k))
    keep = keep_of(odd, first, second, weights[2], parts, give[0].shape)
    keep = across(keep)
    give = sum(x.astype(F32) for x in given).astype(BF)
    taken = lax.ppermute(give, "expert", swap_pair)
    both = jnp.sum(keep.astype(F32), axis=0) + taken.astype(F32)
    both = both.astype(BF).reshape(arrived.shape)
    back = along(both)
    return mixed_of(route, back, rows, block)


def swaps(parts):
    return sorted(range(1, parts), key=lambda k: k == parts // 2)


def solution(mesh):
    spread = P(("group", "expert", "sub"), None)
    weights = P("expert", ("tensor", "sub"), None)
    return jax.shard_map(
        shards,
        mesh=mesh,
        in_specs=(spread, spread, spread, weights, weights, weights),
        out_specs=P(("group", "expert", "sub"), "tensor"),
        check_vma=False,
    )
```

```python
import jax
import jax.numpy as jnp
from jax import lax
from jax.experimental import pallas as pl
from jax.experimental.pallas import tpu as pltpu
from jax.sharding import PartitionSpec as P

BF = jnp.bfloat16
F32 = jnp.float32
I32 = jnp.int32
VM = pl.BlockSpec(memory_space=pltpu.VMEM)
SM = pl.BlockSpec(memory_space=pltpu.SMEM)
ANY = pl.BlockSpec(memory_space=pl.ANY)
CONTRACT = (((1,), (1,)), ((), ()))
MIB = 1024 * 1024


def params(mib):
    return pltpu.CompilerParams(vmem_limit_bytes=mib * MIB)


def split_of(half):
    return -(-half // 256) * 128


def routing(ids_ref, rows, axis):
    shape = (rows, 1) if axis == 0 else (1, rows)
    row = lax.broadcasted_iota(I32, shape, axis)
    expert, side, part = row // 4, (row // 2) % 2, row % 2
    tokens, picks = ids_ref.shape
    count = jnp.zeros(shape, I32)
    out = []
    for t in range(tokens):
        hits = [(expert == ids_ref[t, j]).astype(I32) for j in range(picks)]
        named = sum(hits)
        first = named * (count == part).astype(I32)
        third = named * (count == 2).astype(I32)
        out.append((hits, first, third))
        count = count + named
    return out, side, part


def pack_kernel(here_ref, ids_hbm, tok_hbm, o_ref, ids_ref, tok_ref, sems):
    owners, _, width = o_ref.shape
    rows = 2 * owners
    block = tok_ref.shape[1]
    half = block // 2
    low = width - half
    start = pl.multiple_of(here_ref[0] * block, 128)
    take_ids = pltpu.make_async_copy(ids_hbm, ids_ref, sems.at[0])
    take_tok = pltpu.make_async_copy(tok_hbm.at[:, pl.ds(start, block)], tok_ref, sems.at[1])
    take_ids.start()
    take_tok.start()
    take_ids.wait()
    routes, side, part = routing(ids_ref, rows, 0)
    take_tok.wait()
    tok = tok_ref[...].astype(F32)
    main = jnp.zeros((rows, half), F32)
    tail = jnp.zeros((rows, low), F32)
    for t, (_, first, third) in enumerate(routes):
        for p in range(2):
            piece = tok[t : t + 1, p * half : (p + 1) * half]
            here = (side == p).astype(I32)
            main = main + (first * here).astype(F32) * piece
            rest = piece[:, low:]
            if 2 * low > half:
                rest = jnp.concatenate([rest, jnp.zeros((1, 2 * low - half), F32)], axis=1)
            third_here = third * here
            tail = tail + (third_here * (1 - part)).astype(F32) * piece[:, :low]
            tail = tail + (third_here * part).astype(F32) * rest
    o_ref[:, :, :half] = main.astype(BF).reshape(owners, 2, half)
    o_ref[:, :, half:] = tail.astype(BF).reshape(owners, 2, low)


def in_hbm(x):
    return pltpu.with_memory_space_constraint(x, pltpu.MemorySpace.HBM)


def packed_of(here, ids, tokens, owners, block):
    half = block // 2
    width = half + split_of(half)
    return pl.pallas_call(
        pack_kernel,
        out_shape=jax.ShapeDtypeStruct((owners, 2, width), BF),
        in_specs=[SM, ANY, ANY],
        out_specs=VM,
        scratch_shapes=[
            pltpu.SMEM(ids.shape, I32),
            pltpu.VMEM((tokens.shape[0], block), BF),
            pltpu.SemaphoreType.DMA((2,)),
        ],
        compiler_params=params(4),
        name="pack",
    )(here, in_hbm(ids), in_hbm(tokens))


def route_kernel(ids_ref, code_ref, w_ref):
    routes, side, part = routing(ids_ref, w_ref.shape[1], 1)
    mains, lowers, uppers = [], [], []
    for p in range(2):
        for t, (hits, first, third) in enumerate(routes):
            code = sum(hit * code_ref[t, j] for j, hit in enumerate(hits))
            code = code * (side == p).astype(I32)
            mains.append(first * code)
            lowers.append(third * (1 - part) * code)
            uppers.append(third * part * code)
    weights = jnp.concatenate(mains + lowers + uppers, axis=0).astype(F32) / 64.0
    w_ref[...] = weights.astype(BF)


def route_of(ids, codes, owners):
    return pl.pallas_call(
        route_kernel,
        out_shape=jax.ShapeDtypeStruct((6 * ids.shape[0], 2 * owners), BF),
        in_specs=[SM, SM],
        out_specs=VM,
        compiler_params=params(4),
        name="route",
    )(ids, codes)


def mix_kernel(w_ref, x_ref, o_ref):
    owners, _, width = x_ref.shape
    tokens = o_ref.shape[0]
    half = o_ref.shape[1] // 2
    low = width - half
    x = x_ref[...].reshape(2 * owners, width)
    r = jnp.dot(w_ref[...], x, preferred_element_type=F32)
    n = 2 * tokens
    for p in range(2):
        at, main = p * half, r[p * tokens : (p + 1) * tokens, :half]
        lower = r[n + p * tokens : n + (p + 1) * tokens, half:]
        upper = r[2 * n + p * tokens : 2 * n + (p + 1) * tokens, half : 2 * half - low]
        o_ref[:, at : at + low] = (main[:, :low] + lower).astype(BF)
        o_ref[:, at + low : at + half] = (main[:, low:] + upper).astype(BF)


def mixed_of(weights, x, tokens, block):
    return pl.pallas_call(
        mix_kernel,
        out_shape=jax.ShapeDtypeStruct((tokens, block), BF),
        in_specs=[VM, VM],
        out_specs=VM,
        compiler_params=params(4),
        name="mix",
    )(weights, x)


def start_of(here, odd, half, k, other, turned):
    side = 1 - odd if other else odd
    k = lax.bitwise_xor(here, jnp.int32(k)) if turned else k
    return pl.multiple_of((2 * k + side) * half, 128)


def halves_of(x, half):
    width = x.shape[-1]
    low = width - half
    x = x.reshape(-1, width)
    return (
        (0, low, jnp.concatenate([x[:, :low], x[:, half:]], axis=0)),
        (low, half - low, jnp.concatenate([x[:, low:half], x[:, half : 2 * half - low]], axis=0)),
    )


def add_in(sums, x, at, w_ref, half):
    return [
        total
        + lax.dot_general(
            lhs,
            w_ref[:, pl.ds(pl.multiple_of(at + lo, 128), size)],
            CONTRACT,
            preferred_element_type=F32,
        )
        for total, (lo, size, lhs) in zip(sums, halves_of(x, half))
    ]


def own_kernel(here_ref, odd_ref, *refs):
    own_ref, g0, u0, d0, g1, u1, d1, g_ref, u_ref, d_ref, s_ref, sems = refs
    parts = own_ref.shape[0]
    half = d_ref.shape[1] // (2 * parts)
    copies = []
    for i, (pair, dst) in enumerate((((g0, g1), g_ref), ((u0, u1), u_ref), ((d0, d1), d_ref))):
        for c, src in enumerate(pair):
            units = src.shape[0]
            rows = pl.ds(c * units, units)
            copies.append(pltpu.make_async_copy(src, dst.at[rows], sems.at[2 * i + c]))
    for copy in copies:
        copy.start()
    for i, w_ref in enumerate((g_ref, u_ref)):
        copies[2 * i].wait()
        copies[2 * i + 1].wait()
        sums = [jnp.zeros(s_ref.shape[1:], F32)] * 2
        for k in range(parts):
            at = start_of(here_ref[0], odd_ref[0], half, k, False, False)
            sums = add_in(sums, own_ref[k], at, w_ref, half)
        s_ref[2 * i] = sums[0]
        s_ref[2 * i + 1] = sums[1]
    copies[4].wait()
    copies[5].wait()


def own_part(here, odd, own, mine, theirs):
    _, owners, _, _ = own.shape
    units, features = mine[0].shape
    shape = jax.ShapeDtypeStruct((2 * units, features), BF)
    return pl.pallas_call(
        own_kernel,
        out_shape=(shape,) * 3 + (jax.ShapeDtypeStruct((4, 4 * owners, 2 * units), F32),),
        in_specs=[SM, SM, VM] + [ANY] * 6,
        out_specs=(VM,) * 4,
        scratch_shapes=[pltpu.SemaphoreType.DMA((6,))],
        cost_estimate=pl.CostEstimate(
            flops=16 * owners * units * features,
            bytes_accessed=24 * units * features,
            transcendentals=0,
        ),
        compiler_params=params(16),
        name="ownpart",
    )(here, odd, own, *(in_hbm(w) for w in mine), *theirs)


def expert_kernel(here_ref, odd_ref, s_ref, *refs):
    parts = (len(refs) - 5) // 2
    pals, (g_ref, u_ref, d_ref, a_ref, b_ref) = refs[:parts], refs[parts : parts + 5]
    give_refs = refs[parts + 5 :]
    owners = pals[0].shape[0]
    rows = 2 * owners
    half = d_ref.shape[1] // (2 * parts)
    odd, here = odd_ref[0], here_ref[0]

    gates, ups = [s_ref[0], s_ref[1]], [s_ref[2], s_ref[3]]
    for i, x_ref in enumerate(pals):
        at = start_of(here, odd, half, i, True, True)
        gates = add_in(gates, x_ref[...], at, g_ref, half)
        ups = add_in(ups, x_ref[...], at, u_ref, half)

    def joined(a, b):
        third = a[rows:] + pltpu.roll(b[rows:], rows - 1, 0)
        return jnp.concatenate([a[:rows] + b[:rows], third], axis=0)

    gate, up = joined(*gates), joined(*ups)
    hidden = gate / (1.0 + jnp.exp(-gate)) * up
    third = hidden[rows:]
    even = lax.broadcasted_iota(I32, third.shape, 0) % 2 == 0
    lower = jnp.where(even, third, 0.0)
    upper = jnp.where(even, 0.0, pltpu.roll(third, 1, 0))
    a_ref[...] = jnp.concatenate([hidden[:rows], lower], axis=0).astype(BF)
    b_ref[...] = jnp.concatenate([hidden[:rows], upper], axis=0).astype(BF)
    for k in range(parts):
        at = start_of(here, odd, half, k, True, True)
        down_into(give_refs[k], a_ref[...], b_ref[...], d_ref, at, half)


def down_into(o_ref, first, second, d_ref, at, half, extra=None):
    rows, width = o_ref.shape
    low = width - half
    a = jnp.dot(first, d_ref[:, pl.ds(at, low)], preferred_element_type=F32)
    cols = pl.ds(pl.multiple_of(at + low, 128), half - low)
    b = jnp.dot(second, d_ref[:, cols], preferred_element_type=F32)

    def put(lo, value):
        hi = lo + value.shape[1]
        if extra is not None:
            value = value + extra[:, lo:hi].astype(F32)
        o_ref[:, lo:hi] = value.astype(BF)

    put(0, a[:rows])
    put(low, b[:rows])
    put(half, a[rows:, : half - low] + b[rows:])
    if 2 * low > half:
        put(2 * half - low, a[rows:, half - low :])


def keep_body(far, here_ref, odd_ref, a_ref, b_ref, extra_ref, d_ref, o_ref):
    parts = o_ref.shape[0]
    half = d_ref.shape[1] // (2 * parts)
    here = here_ref[0]
    for k in range(parts):
        at = start_of(here, odd_ref[0], half, k, False, True)
        extra = extra_ref[...] if k == far else None
        block = o_ref.at[lax.bitwise_xor(here, jnp.int32(k))]
        down_into(block, a_ref[...], b_ref[...], d_ref, at, half, extra)


def experts_of(here, odd, sums, pals, weights):
    parts = len(pals)
    owners, _, width = pals[0].shape
    units, features = weights[0].shape
    lhs = jax.ShapeDtypeStruct((4 * owners, units), BF)
    one = jax.ShapeDtypeStruct((2 * owners, width), BF)
    a, b, *give = pl.pallas_call(
        expert_kernel,
        out_shape=(lhs, lhs, *(one,) * parts),
        in_specs=[SM] * 2 + [VM] * (parts + 4),
        out_specs=(VM,) * (parts + 2),
        cost_estimate=pl.CostEstimate(
            flops=12 * owners * units * features,
            bytes_accessed=6 * units * features,
            transcendentals=4 * owners * units,
        ),
        compiler_params=params(24),
        name="experts",
    )(here, odd, sums, *pals, *weights)
    return a, b, give


def keep_of(here, odd, far, a, b, extra, down, parts):
    def kernel(*refs):
        keep_body(far, *refs)

    return pl.pallas_call(
        kernel,
        out_shape=jax.ShapeDtypeStruct((parts, *extra.shape), BF),
        in_specs=[SM, SM, VM, VM, VM, VM],
        out_specs=VM,
        cost_estimate=pl.CostEstimate(
            flops=a.size * down.shape[1],
            bytes_accessed=2 * down.size,
            transcendentals=0,
        ),
        compiler_params=params(24),
        name="keepdown",
    )(here, odd, a, b, extra, down)


def shards(tokens, expert_ids, gate_codes, w_gate, w_up, w_down):
    rows, features = tokens.shape
    owners = lax.axis_size("expert")
    subs = lax.axis_size("sub")
    parts = lax.axis_size("tensor")
    experts = owners // 2
    assert min(rows, rows * expert_ids.shape[1] // experts + 1) == 3
    block = features // parts
    here = lax.axis_index("tensor").reshape(1)
    odd = (lax.axis_index("expert") & 1).reshape(1)
    swap_sub = [(i, subs - 1 - i) for i in range(subs)]
    swap_pair = [(i, i ^ 1) for i in range(owners)]

    def swapped(x, k):
        return lax.ppermute(x, "tensor", [(i, i ^ k) for i in range(parts)])

    def across(x):
        return lax.all_to_all(x, "tensor", split_axis=0, concat_axis=0, tiled=True)

    def along(x):
        return lax.all_to_all(x, "expert", split_axis=0, concat_axis=0, tiled=True)

    own = (w_gate[0], w_up[0], w_down[0])
    other = [lax.ppermute(w, "sub", swap_sub) for w in own]
    packed = packed_of(here, expert_ids, tokens, owners, block)
    arrived = along(packed)
    route = route_of(expert_ids, gate_codes, owners)
    partner = lax.ppermute(arrived, "expert", swap_pair)
    spread = jnp.broadcast_to(arrived[None], (parts, *arrived.shape))
    spread = across(spread)
    far, near = swaps(parts)
    pals = {0: partner}
    for k in near:
        pals[k] = swapped(partner, k)
    pals[far] = swapped(partner, far)
    pals = [pals[k] for k in range(parts)]
    *weights, sums = own_part(here, odd, spread, own, other)
    first, second, give = experts_of(here, odd, sums, pals, weights)
    extra = lax.ppermute(give[far], "expert", swap_pair)
    given = [give[0]]
    for k in near:
        given.append(swapped(give[k], k))
    keep = keep_of(here, odd, far, first, second, extra, weights[2], parts)
    keep = across(keep)
    give = sum(x.astype(F32) for x in given).astype(BF)
    taken = lax.ppermute(give, "expert", swap_pair)
    both = jnp.sum(keep.astype(F32), axis=0) + taken.astype(F32)
    both = both.astype(BF).reshape(arrived.shape)
    back = along(both)
    return mixed_of(route, back, rows, block)


def swaps(parts):
    far = parts // 2
    return far, [k for k in range(1, parts) if k != far]


def solution(mesh):
    spread = P(("group", "expert", "sub"), None)
    weights = P("expert", ("tensor", "sub"), None)
    return jax.shard_map(
        shards,
        mesh=mesh,
        in_specs=(spread, spread, spread, weights, weights, weights),
        out_specs=P(("group", "expert", "sub"), "tensor"),
        check_vma=False,
    )
```

```python
import jax
import jax.numpy as jnp
from jax import lax
from jax.experimental import pallas as pl
from jax.experimental.pallas import tpu as pltpu
from jax.sharding import PartitionSpec as P

BF = jnp.bfloat16
F32 = jnp.float32
I32 = jnp.int32
VM = pl.BlockSpec(memory_space=pltpu.VMEM)
SM = pl.BlockSpec(memory_space=pltpu.SMEM)
ANY = pl.BlockSpec(memory_space=pl.ANY)
CONTRACT = (((1,), (1,)), ((), ()))
MIB = 1024 * 1024


def params(mib):
    return pltpu.CompilerParams(vmem_limit_bytes=mib * MIB)


def split_of(half):
    return -(-half // 256) * 128


def routing(ids_ref, rows):
    shape = (1, rows)
    row = lax.broadcasted_iota(I32, shape, 1)
    expert, side, part = row // 4, (row // 2) % 2, row % 2
    tokens, picks = ids_ref.shape
    count = jnp.zeros(shape, I32)
    out = []
    for t in range(tokens):
        hits = [(expert == ids_ref[t, j]).astype(I32) for j in range(picks)]
        named = sum(hits)
        first = named * (count == part).astype(I32)
        third = named * (count == 2).astype(I32)
        out.append((hits, first, third))
        count = count + named
    return out, side, part


def pack_kernel(here_ref, ids_hbm, tok_hbm, o_ref, ids_ref, tok_ref, sems):
    owners, _, width = o_ref.shape
    rows = 2 * owners
    block = tok_ref.shape[1]
    half = block // 2
    low = width - half
    start = pl.multiple_of(here_ref[0] * block, 128)
    take_ids = pltpu.make_async_copy(ids_hbm, ids_ref, sems.at[0])
    take_tok = pltpu.make_async_copy(tok_hbm.at[:, pl.ds(start, block)], tok_ref, sems.at[1])
    take_ids.start()
    take_tok.start()
    take_ids.wait()
    routes, side, part = routing(ids_ref, rows)
    mains, lowers, uppers = [], [], []
    for p in range(2):
        here = (side == p).astype(I32)
        for _, first, third in routes:
            mains.append(first * here)
            lowers.append(third * here * (1 - part))
            uppers.append(third * here * part)
    main, tail = (
        jnp.concatenate(x, axis=0).astype(F32).astype(BF) for x in (mains, lowers + uppers)
    )
    take_tok.wait()
    tok = tok_ref[...].astype(F32)
    both = jnp.concatenate([tok[:, :half], tok[:, half:]], axis=0)
    rest = both[:, low:]
    if 2 * low > half:
        rest = jnp.concatenate([rest, jnp.zeros((rest.shape[0], 2 * low - half), F32)], axis=1)
    ends = jnp.concatenate([both[:, :low], rest], axis=0)
    pick = (((0,), (0,)), ((), ()))
    main = lax.dot_general(main, both.astype(BF), pick, preferred_element_type=F32)
    tail = lax.dot_general(tail, ends.astype(BF), pick, preferred_element_type=F32)
    o_ref[:, :, :half] = main.astype(BF).reshape(owners, 2, half)
    o_ref[:, :, half:] = tail.astype(BF).reshape(owners, 2, low)


def in_hbm(x):
    return pltpu.with_memory_space_constraint(x, pltpu.MemorySpace.HBM)


def packed_of(here, ids, tokens, owners, block):
    half = block // 2
    width = half + split_of(half)
    return pl.pallas_call(
        pack_kernel,
        out_shape=jax.ShapeDtypeStruct((owners, 2, width), BF),
        in_specs=[SM, ANY, ANY],
        out_specs=VM,
        scratch_shapes=[
            pltpu.SMEM(ids.shape, I32),
            pltpu.VMEM((tokens.shape[0], block), BF),
            pltpu.SemaphoreType.DMA((2,)),
        ],
        compiler_params=params(4),
        name="pack",
    )(here, in_hbm(ids), in_hbm(tokens))


def route_kernel(ids_ref, code_ref, w_ref):
    routes, side, part = routing(ids_ref, w_ref.shape[1])
    mains, lowers, uppers = [], [], []
    for p in range(2):
        for t, (hits, first, third) in enumerate(routes):
            code = sum(hit * code_ref[t, j] for j, hit in enumerate(hits))
            code = code * (side == p).astype(I32)
            mains.append(first * code)
            lowers.append(third * (1 - part) * code)
            uppers.append(third * part * code)
    weights = jnp.concatenate(mains + lowers + uppers, axis=0).astype(F32) / 64.0
    w_ref[...] = weights.astype(BF)


def route_of(ids, codes, owners):
    return pl.pallas_call(
        route_kernel,
        out_shape=jax.ShapeDtypeStruct((6 * ids.shape[0], 2 * owners), BF),
        in_specs=[SM, SM],
        out_specs=VM,
        compiler_params=params(4),
        name="route",
    )(ids, codes)


def mix_kernel(w_ref, x_ref, o_ref):
    owners, _, width = x_ref.shape
    tokens = o_ref.shape[0]
    half = o_ref.shape[1] // 2
    low = width - half
    x = x_ref[...].reshape(2 * owners, width)
    r = jnp.dot(w_ref[...], x, preferred_element_type=F32)
    n = 2 * tokens
    for p in range(2):
        at, main = p * half, r[p * tokens : (p + 1) * tokens, :half]
        lower = r[n + p * tokens : n + (p + 1) * tokens, half:]
        upper = r[2 * n + p * tokens : 2 * n + (p + 1) * tokens, half : 2 * half - low]
        o_ref[:, at : at + low] = (main[:, :low] + lower).astype(BF)
        o_ref[:, at + low : at + half] = (main[:, low:] + upper).astype(BF)


def mixed_of(weights, x, tokens, block):
    return pl.pallas_call(
        mix_kernel,
        out_shape=jax.ShapeDtypeStruct((tokens, block), BF),
        in_specs=[VM, VM],
        out_specs=VM,
        compiler_params=params(4),
        name="mix",
    )(weights, x)


def start_of(here, odd, half, k, other, turned):
    side = 1 - odd if other else odd
    k = lax.bitwise_xor(here, jnp.int32(k)) if turned else k
    return pl.multiple_of((2 * k + side) * half, 128)


def halves_of(x, half):
    width = x.shape[-1]
    low = width - half
    x = x.reshape(-1, width)
    return (
        (0, low, jnp.concatenate([x[:, :low], x[:, half:]], axis=0)),
        (low, half - low, jnp.concatenate([x[:, low:half], x[:, half : 2 * half - low]], axis=0)),
    )


def add_in(sums, x, at, w_ref, half):
    return [
        total
        + lax.dot_general(
            lhs,
            w_ref[:, pl.ds(pl.multiple_of(at + lo, 128), size)],
            CONTRACT,
            preferred_element_type=F32,
        )
        for total, (lo, size, lhs) in zip(sums, halves_of(x, half))
    ]


def own_kernel(here_ref, odd_ref, *refs):
    own_ref, g0, u0, d0, g1, u1, d1, g_ref, u_ref, d_ref, s_ref, sems = refs
    parts = own_ref.shape[0]
    half = d_ref.shape[1] // (2 * parts)
    copies = []
    for i, (pair, dst) in enumerate((((g0, g1), g_ref), ((u0, u1), u_ref), ((d0, d1), d_ref))):
        for c, src in enumerate(pair):
            units = src.shape[0]
            rows = pl.ds(c * units, units)
            copies.append(pltpu.make_async_copy(src, dst.at[rows], sems.at[2 * i + c]))
    for copy in copies:
        copy.start()
    for i, w_ref in enumerate((g_ref, u_ref)):
        copies[2 * i].wait()
        copies[2 * i + 1].wait()
        sums = [jnp.zeros(s_ref.shape[1:], F32)] * 2
        for k in range(parts):
            at = start_of(here_ref[0], odd_ref[0], half, k, False, False)
            sums = add_in(sums, own_ref[k], at, w_ref, half)
        s_ref[2 * i] = sums[0]
        s_ref[2 * i + 1] = sums[1]
    copies[4].wait()
    copies[5].wait()


def own_part(here, odd, own, mine, theirs):
    _, owners, _, _ = own.shape
    units, features = mine[0].shape
    shape = jax.ShapeDtypeStruct((2 * units, features), BF)
    return pl.pallas_call(
        own_kernel,
        out_shape=(shape,) * 3 + (jax.ShapeDtypeStruct((4, 4 * owners, 2 * units), F32),),
        in_specs=[SM, SM, VM] + [ANY] * 6,
        out_specs=(VM,) * 4,
        scratch_shapes=[pltpu.SemaphoreType.DMA((6,))],
        cost_estimate=pl.CostEstimate(
            flops=16 * owners * units * features,
            bytes_accessed=24 * units * features,
            transcendentals=0,
        ),
        compiler_params=params(16),
        name="ownpart",
    )(here, odd, own, *(in_hbm(w) for w in mine), *theirs)


def expert_kernel(here_ref, odd_ref, s_ref, *refs):
    parts = (len(refs) - 5) // 2
    pals, (g_ref, u_ref, d_ref, a_ref, b_ref) = refs[:parts], refs[parts : parts + 5]
    give_refs = refs[parts + 5 :]
    owners = pals[0].shape[0]
    rows = 2 * owners
    half = d_ref.shape[1] // (2 * parts)
    odd, here = odd_ref[0], here_ref[0]

    gates, ups = [s_ref[0], s_ref[1]], [s_ref[2], s_ref[3]]
    for i, x_ref in enumerate(pals):
        at = start_of(here, odd, half, i, True, True)
        gates = add_in(gates, x_ref[...], at, g_ref, half)
        ups = add_in(ups, x_ref[...], at, u_ref, half)

    def joined(a, b):
        third = a[rows:] + pltpu.roll(b[rows:], rows - 1, 0)
        return jnp.concatenate([a[:rows] + b[:rows], third], axis=0)

    gate, up = joined(*gates), joined(*ups)
    hidden = gate / (1.0 + jnp.exp(-gate)) * up
    third = hidden[rows:]
    even = lax.broadcasted_iota(I32, third.shape, 0) % 2 == 0
    lower = jnp.where(even, third, 0.0)
    upper = jnp.where(even, 0.0, pltpu.roll(third, 1, 0))
    a_ref[...] = jnp.concatenate([hidden[:rows], lower], axis=0).astype(BF)
    b_ref[...] = jnp.concatenate([hidden[:rows], upper], axis=0).astype(BF)
    for k in range(parts):
        at = start_of(here, odd, half, k, True, True)
        down_into(give_refs[k], a_ref[...], b_ref[...], d_ref, at, half)


def down_into(o_ref, first, second, d_ref, at, half, extra=None):
    rows, width = o_ref.shape
    low = width - half
    a = jnp.dot(first, d_ref[:, pl.ds(at, low)], preferred_element_type=F32)
    cols = pl.ds(pl.multiple_of(at + low, 128), half - low)
    b = jnp.dot(second, d_ref[:, cols], preferred_element_type=F32)

    def put(lo, value):
        hi = lo + value.shape[1]
        if extra is not None:
            value = value + extra[:, lo:hi].astype(F32)
        o_ref[:, lo:hi] = value.astype(BF)

    put(0, a[:rows])
    put(low, b[:rows])
    put(half, a[rows:, : half - low] + b[rows:])
    if 2 * low > half:
        put(2 * half - low, a[rows:, half - low :])


def keep_body(far, here_ref, odd_ref, a_ref, b_ref, extra_ref, d_ref, o_ref):
    parts = o_ref.shape[0]
    half = d_ref.shape[1] // (2 * parts)
    here = here_ref[0]
    for k in range(parts):
        at = start_of(here, odd_ref[0], half, k, False, True)
        extra = extra_ref[...] if k == far else None
        block = o_ref.at[lax.bitwise_xor(here, jnp.int32(k))]
        down_into(block, a_ref[...], b_ref[...], d_ref, at, half, extra)


def experts_of(here, odd, sums, pals, weights):
    parts = len(pals)
    owners, _, width = pals[0].shape
    units, features = weights[0].shape
    lhs = jax.ShapeDtypeStruct((4 * owners, units), BF)
    one = jax.ShapeDtypeStruct((2 * owners, width), BF)
    a, b, *give = pl.pallas_call(
        expert_kernel,
        out_shape=(lhs, lhs, *(one,) * parts),
        in_specs=[SM] * 2 + [VM] * (parts + 4),
        out_specs=(VM,) * (parts + 2),
        cost_estimate=pl.CostEstimate(
            flops=12 * owners * units * features,
            bytes_accessed=6 * units * features,
            transcendentals=4 * owners * units,
        ),
        compiler_params=params(24),
        name="experts",
    )(here, odd, sums, *pals, *weights)
    return a, b, give


def keep_of(here, odd, far, a, b, extra, down, parts):
    def kernel(*refs):
        keep_body(far, *refs)

    return pl.pallas_call(
        kernel,
        out_shape=jax.ShapeDtypeStruct((parts, *extra.shape), BF),
        in_specs=[SM, SM, VM, VM, VM, VM],
        out_specs=VM,
        cost_estimate=pl.CostEstimate(
            flops=a.size * down.shape[1],
            bytes_accessed=2 * down.size,
            transcendentals=0,
        ),
        compiler_params=params(24),
        name="keepdown",
    )(here, odd, a, b, extra, down)


def shards(tokens, expert_ids, gate_codes, w_gate, w_up, w_down):
    rows, features = tokens.shape
    owners = lax.axis_size("expert")
    subs = lax.axis_size("sub")
    parts = lax.axis_size("tensor")
    experts = owners // 2
    assert min(rows, rows * expert_ids.shape[1] // experts + 1) == 3
    block = features // parts
    here = lax.axis_index("tensor").reshape(1)
    odd = (lax.axis_index("expert") & 1).reshape(1)
    swap_sub = [(i, subs - 1 - i) for i in range(subs)]
    swap_pair = [(i, i ^ 1) for i in range(owners)]

    def swapped(x, k):
        return lax.ppermute(x, "tensor", [(i, i ^ k) for i in range(parts)])

    def across(x):
        return lax.all_to_all(x, "tensor", split_axis=0, concat_axis=0, tiled=True)

    def along(x):
        return lax.all_to_all(x, "expert", split_axis=0, concat_axis=0, tiled=True)

    own = (w_gate[0], w_up[0], w_down[0])
    other = [lax.ppermute(w, "sub", swap_sub) for w in own]
    packed = packed_of(here, expert_ids, tokens, owners, block)
    arrived = along(packed)
    route = route_of(expert_ids, gate_codes, owners)
    partner = lax.ppermute(arrived, "expert", swap_pair)
    spread = jnp.broadcast_to(arrived[None], (parts, *arrived.shape))
    spread = across(spread)
    far, near = swaps(parts)
    pals = {0: partner}
    for k in near:
        pals[k] = swapped(partner, k)
    pals[far] = swapped(partner, far)
    pals = [pals[k] for k in range(parts)]
    *weights, sums = own_part(here, odd, spread, own, other)
    first, second, give = experts_of(here, odd, sums, pals, weights)
    extra = lax.ppermute(give[far], "expert", swap_pair)
    given = [give[0]]
    for k in near:
        given.append(swapped(give[k], k))
    keep = keep_of(here, odd, far, first, second, extra, weights[2], parts)
    keep = across(keep)
    give = sum(x.astype(F32) for x in given).astype(BF)
    taken = lax.ppermute(give, "expert", swap_pair)
    both = jnp.sum(keep.astype(F32), axis=0) + taken.astype(F32)
    both = both.astype(BF).reshape(arrived.shape)
    back = along(both)
    return mixed_of(route, back, rows, block)


def swaps(parts):
    far = parts // 2
    return far, [k for k in range(1, parts) if k != far]


def solution(mesh):
    spread = P(("group", "expert", "sub"), None)
    weights = P("expert", ("tensor", "sub"), None)
    return jax.shard_map(
        shards,
        mesh=mesh,
        in_specs=(spread, spread, spread, weights, weights, weights),
        out_specs=P(("group", "expert", "sub"), "tensor"),
        check_vma=False,
    )
```
